128 devices in a mesh: gx: 4 (over x), gy: 4 (over y), gz: 8 (over z, core).
Axes of the slice: x: 4, y: 4, z: 4, core: 2. Of those that a mesh axis runs over, the one named last changes fastest.
Arguments:
- fields: bfloat16 [16384, 2048], P(('gx', 'gy', 'gz')), may hold values from -6 to 6
- coordinates: float32 [3, 2097152], P(None, ('gx', 'gy', 'gz')), may hold values from -1 to 1
- element_rank: int32 [2097152, 1], P(('gx', 'gy', 'gz')), may hold values from 0 to 127; in each aligned block of 16384 rows (0 to 16383, 16384 to 32767, ...) at most 160 rows name the same one
- element_slot: int32 [2097152], P(('gx', 'gy', 'gz')), may hold values from 0 to 127
Outputs:
- samples: float32 [4, 2097152], P(None, ('gx', 'gy', 'gz'))
The draws below stay inside these ranges and needn't reach their ends.
Inputs may be any that keep to these rules, and one draw needn't show every extreme that they name: `element_rank`: among the probes of one device no rank is named by more than 160 probes, and in some devices' blocks one rank is named by exactly 160.
All inputs are finite; a program needn't handle non-finite values.
Results may differ from the reference program's by a relative error of at most 0.0024.
Values sent between devices are 32-bit elements; how exact they have to be, the bound alone decides.
A program may use at most 64 MiB of HBM per device.

```python
import math
import jax
import jax.numpy as jnp
import numpy as np
from jax import lax

ROW = 2048
E_DEV = 128
P_DEV = 16384
CAP = 160
ELEMENTS = 16384
PROBES = 2097152
DEVICES = 128


def place_ends(values, key, least, largest):
    longest = values.shape.index(max(values.shape))
    spots = []
    for shift in (0, 1):
        where = [jax.random.randint(jax.random.fold_in(key, axis), (), 0, length) for axis, length in enumerate(values.shape)]
        where[longest] = (where[longest] + shift) % values.shape[longest]
        spots.append(tuple(where))
    return values.at[spots[0]].set(least).at[spots[1]].set(largest)


def shard_levels(rng, dims, split, least, largest):
    loudness = 1.0
    for axis_at, parts in split:
        heights = jax.random.uniform(jax.random.fold_in(jax.random.fold_in(rng, 6), axis_at), (parts,), jnp.float32, least / len(split), largest / len(split))
        loudness = loudness * jnp.repeat(jnp.exp(heights), dims[axis_at] // parts).reshape((-1,) + (1,) * (len(dims) - 1 - axis_at))
    return loudness


def routed_block(key, own, number, rows, count, top, most, slope):
    sequence = jax.random.permutation(key, count)
    packed, usual = shares(count, rows * top, most, slope, True), shares(count, rows * top, most, slope, False)
    places = jnp.arange(count)

    def named(sizes, turn):
        used = int((sizes > 0).sum())
        fixed = max(1, used // 4)
        shifted = fixed + (places - fixed + turn * (used - fixed)) % max(1, count - fixed)
        return jnp.zeros((count,), jnp.int32).at[sequence[jnp.where(places < fixed, places, shifted)]].set(jnp.asarray(sizes, jnp.int32))

    sizes = jnp.where(number % 4 == 0, named(packed, number // 4), named(usual, number - number // 4 - 1))
    mixed = jax.random.permutation(jax.random.fold_in(own, 3), count)
    source_of, sink = mixed[0:count // 2 * 2:2], mixed[1:count // 2 * 2:2]
    margin = jnp.minimum(sizes[source_of] - 1, most - sizes[sink]) // 2
    margin = jnp.where((source_of == sequence[0]) | (sink == sequence[0]) | (sizes[sink] == 0), 0, jnp.maximum(margin, 0))
    shifted = jax.random.randint(jax.random.fold_in(own, 4), (count // 2,), 0, 1 << 20) % (margin + 1)
    sizes = sizes.at[source_of].add(-shifted).at[sink].add(shifted)
    labels = jnp.searchsorted(jnp.cumsum(sizes), jnp.arange(rows * top), side="right").astype(jnp.int32)
    listing = labels.reshape(top, rows).T
    listing = listing[jax.random.permutation(jax.random.fold_in(own, 1), rows)]
    turn = jax.random.randint(jax.random.fold_in(own, 2), (rows, 1), 0, top)
    return jnp.take_along_axis(listing, (jnp.arange(top)[None, :] + turn) % top, axis=1)


def shares(count, total, bound, skew, full):
    loads = [(1 << 20) // math.isqrt(standing ** skew) + 1 for standing in range(1, count + 1)]
    largest = bound if full else min(bound, max(-(-total // count), total * loads[0] // sum(loads)))
    least = 1 if total - largest >= count - 1 else 0
    given, rest = [largest] + [least] * (count - 1), total - largest - least * (count - 1)
    while rest > 0:
        free = [i for i in range(1, count) if given[i] < largest] or [i for i in range(1, count) if given[i] < bound]
        pool, remaining = sum([loads[i] for i in free]), rest
        for i in free:
            addition = min(bound - given[i], max(1, remaining * loads[i] // pool), rest)
            given[i] = given[i] + addition
            rest = rest - addition
    return np.array(given)


def bell_draw(own_key, extent, spread, most, shards=(), held_as=jnp.bfloat16):
    drawn = jax.random.normal(own_key, extent, jnp.float32) * spread
    if len(shards) > 0:
        drawn = shard_levels(own_key, extent, shards, -0.22, 0.18) * drawn
    return jnp.clip(drawn, min=-most, max=most).astype(held_as)


def setup_inputs(seed: int = 0) -> dict:
    arg_keys = jax.random.split(jax.random.key(seed), 5)
    fields = bell_draw(arg_keys[0], (ELEMENTS, ROW), 1.0, 6.0, ((0, 128),))
    coordinates = jnp.clip(jax.random.uniform(arg_keys[1], (3, PROBES), jnp.float32, -1.0, 1.0) * shard_levels(arg_keys[1], (3, PROBES), ((1, 128),), -0.4, 0.0), -1.0, 1.0)
    element_rank_keys = jax.random.split(jax.random.fold_in(arg_keys[2], 1), PROBES // P_DEV)
    element_rank_turns = jax.random.permutation(jax.random.fold_in(arg_keys[2], 3), PROBES // P_DEV)
    element_rank = jax.vmap(lambda own, number: routed_block(jax.random.fold_in(arg_keys[2], 2), own, number, P_DEV, DEVICES, 1, CAP, 2))(element_rank_keys, element_rank_turns).reshape((PROBES, 1))
    element_slot = place_ends(jax.random.randint(arg_keys[3], (PROBES,), 0, E_DEV), jax.random.fold_in(arg_keys[3], 1), 0, E_DEV - 1).astype(jnp.int32)
    return {"fields": fields, "coordinates": coordinates, "element_rank": element_rank, "element_slot": element_slot}


gll_points = np.array([-1.0, -0.8717401485096066, -0.5917001814331423, -0.2092992179024789, 0.2092992179024789, 0.5917001814331423, 0.8717401485096066, 1.0])
gll_scale = np.array([1.0 / np.prod([gll_points[a] - gll_points[b] for b in range(8) if b != a]) for a in range(8)])


def lagrange(coord):
    offsets = coord[None, :] - jnp.asarray(gll_points, coord.dtype)[:, None]
    weights = []
    for node_a in range(8):
        factor = jnp.ones_like(coord) * gll_scale[node_a]
        for node_b in range(8):
            if node_b != node_a:
                factor = factor * offsets[node_b]
        weights.append(factor)
    return jnp.stack(weights, axis=0)


def interpolate(coordinates, element, fields):
    total_rows = element.shape[0]
    block_rows = math.gcd(total_rows, 8192)
    block_count = total_rows // block_rows

    def one_block(pieces):
        coords_block, slots_block = pieces
        weight_r = lagrange(coords_block[0])
        weight_s = lagrange(coords_block[1])
        weight_t = lagrange(coords_block[2]).astype(jnp.bfloat16)
        gathered = jnp.take(fields, slots_block, axis=0).reshape(block_rows, 256, 8)
        along_t = jnp.einsum("nak,kn->na", gathered.astype(jnp.float32), weight_t.astype(jnp.float32), precision=lax.Precision.HIGHEST)
        along_t = along_t.reshape(block_rows, 4, 8, 8)
        along_s = jnp.einsum("nfij,jn->nfi", along_t, weight_s, precision=lax.Precision.HIGHEST)
        return jnp.einsum("nfi,in->fn", along_s, weight_r, precision=lax.Precision.HIGHEST)

    coords_blocks = coordinates.reshape(3, block_count, block_rows).transpose(1, 0, 2)
    slot_blocks = element.reshape(block_count, block_rows)
    result = lax.map(one_block, (coords_blocks, slot_blocks))
    return result.transpose(1, 0, 2).reshape(4, total_rows)


def reference(fields, coordinates, element_rank, element_slot):
    element = element_rank[:, 0].astype(jnp.int32) * E_DEV + element_slot.astype(jnp.int32)
    return interpolate(coordinates, element, fields)
```

```python
import jax
import jax.numpy as jnp
import numpy as np
from jax import lax
from jax.experimental import pallas as pl
from jax.experimental.pallas import tpu as pltpu
from jax.sharding import PartitionSpec as P

AXES = ("gx", "gy", "gz")
NV = 16

gll_points = np.array(
    [
        -1.0,
        -0.8717401485096066,
        -0.5917001814331423,
        -0.2092992179024789,
        0.2092992179024789,
        0.5917001814331423,
        0.8717401485096066,
        1.0,
    ]
)
gll_scale = np.array(
    [1.0 / np.prod([gll_points[a] - gll_points[b] for b in range(8) if b != a]) for a in range(8)]
)


def iotas():
    return lax.broadcasted_iota(jnp.int32, (8, 128), 0), lax.broadcasted_iota(jnp.int32, (8, 128), 1)


def partner(x, axis, d, bit):
    n = x.shape[axis]
    if 2 * d == n:
        return pltpu.roll(x, d, axis)
    if axis == 1:
        idx = lax.broadcasted_iota(jnp.int32, x.shape, 1) ^ d
        return jnp.take_along_axis(x, idx, axis=1)
    return jnp.where(bit, pltpu.roll(x, d, axis), pltpu.roll(x, n - d, axis))


def network(arrs):
    s_io, l_io = iotas()
    arrs = [list(a) for a in arrs]
    count = len(arrs)

    def bit_of(b):
        if b < 7:
            return ((s_io >> (b - 4)) & 1) == 1
        return ((l_io >> (b - 7)) & 1) == 1

    for k in range(1, 15):
        down = bit_of(k) if 4 <= k < 14 else None
        for j in range(k - 1, 3, -1):
            axis, d = (0, 1 << (j - 4)) if j < 7 else (1, 1 << (j - 7))
            upper = bit_of(j)
            flip = upper if down is None else jnp.logical_xor(upper, down)
            for v in range(NV):
                other = [partner(arrs[a][v], axis, d, upper) for a in range(count)]
                take = jnp.logical_xor(arrs[0][v] > other[0], flip)
                for a in range(count):
                    arrs[a][v] = jnp.where(take, other[a], arrs[a][v])
        for j in range(min(k, 4) - 1, -1, -1):
            d = 1 << j
            for v in range(NV):
                if v & d:
                    continue
                w = v | d
                if k < 4 and (v >> k) & 1:
                    swap = arrs[0][v] < arrs[0][w]
                else:
                    swap = arrs[0][v] > arrs[0][w]
                if down is not None:
                    swap = jnp.logical_xor(swap, down)
                for a in range(count):
                    x, y = arrs[a][v], arrs[a][w]
                    arrs[a][v] = jnp.where(swap, y, x)
                    arrs[a][w] = jnp.where(swap, x, y)
    return arrs


def take_lanes(x, idx):
    return jnp.take_along_axis(x, idx, axis=1)


def rows_up(low, high, d, s_io):
    return jnp.where(s_io < 8 - d, pltpu.roll(low, 8 - d, 0), pltpu.roll(high, 8 - d, 0))


def rows_down(low, high, d, s_io):
    return jnp.where(s_io >= d, pltpu.roll(high, d, 0), pltpu.roll(low, d, 0))


def dispatch_kernel(rank_ref, slot_ref, coord_ref, send_ref, key_ref, meta_ref):
    s_io, l_io = iotas()
    keys = []
    for v in range(NV):
        label = l_io * 128 + s_io * 16 + v
        keys.append(rank_ref[v] * (1 << 21) + slot_ref[v] * (1 << 14) + label)
    coords = [[coord_ref[c, v] for v in range(NV)] for c in range(3)]
    keys, *coords = network([keys] + coords)
    for v in range(NV):
        key_ref[v] = keys[v]
    last = (keys[NV - 1][7:8, :] >> 21).astype(jnp.float32)
    last = jnp.broadcast_to(last, (128, 128)).T
    lanes = lax.broadcasted_iota(jnp.int32, (128, 128), 1).astype(jnp.float32)
    column = jnp.sum((last < lanes).astype(jnp.float32), axis=0, keepdims=True)
    column = jnp.broadcast_to(column, (8, 128)).astype(jnp.int32)
    columns = [jnp.minimum(column + k, 127) for k in range(3)]
    spread = [[take_lanes(keys[v], columns[k]) for v in range(NV)] for k in range(3)]
    below = jnp.zeros((8, 128), jnp.float32)
    for v in range(NV):
        below = below + ((spread[0][v] >> 21) < l_io).astype(jnp.float32)
    shift = jnp.broadcast_to(jnp.sum(below, axis=0, keepdims=True), (8, 128)).astype(jnp.int32)
    meta_ref[0] = column
    meta_ref[1] = shift

    tails = []
    for a in range(4):
        if a == 3:
            table = [[((x >> 14) & 127).astype(jnp.float32) for x in block] for block in spread]
        else:
            table = [[take_lanes(coords[a][v], columns[k]) for v in range(NV)] for k in range(3)]
        for b in range(4):
            d = 1 << b
            bit = ((shift >> b) & 1) == 1
            moved = []
            for k in range(3):
                row = []
                for v in range(NV):
                    if v + d < NV:
                        src = table[k][v + d]
                    else:
                        src = rows_up(table[k][v + d - NV], table[min(k + 1, 2)][v + d - NV], 1, s_io)
                    row.append(jnp.where(bit, src, table[k][v]))
                moved.append(row)
            table = moved
        for b in range(4, 7):
            d = 1 << (b - 4)
            bit = ((shift >> b) & 1) == 1
            moved = [
                [
                    jnp.where(bit, rows_up(table[k][v], table[min(k + 1, len(table) - 1)][v], d, s_io), table[k][v])
                    for v in range(NV)
                ]
                for k in range(2)
            ]
            table = moved
        send_ref[a] = jnp.concatenate(table[0], axis=0).T
        for q in range(4):
            tail = table[1][4 * q]
            for u in range(1, 4):
                tail = jnp.where(s_io >= 2 * u, pltpu.roll(table[1][4 * q + u], 2 * u, 0), tail)
            tails.append(tail)
    send_ref[4] = jnp.concatenate(tails, axis=0).T


def return_kernel(back_ref, key_ref, meta_ref, out_ref):
    s_io, l_io = iotas()
    column, shift = meta_ref[0], meta_ref[1]
    keys = [key_ref[v] for v in range(NV)]
    ranks = [x >> 21 for x in keys]
    blocks = [l_io - take_lanes(column, x) for x in ranks]
    tails = back_ref[4].T
    values = []
    for f in range(4):
        main = back_ref[f].T
        first = [main[8 * v : 8 * v + 8] for v in range(NV)]
        second = []
        for v in range(NV):
            q, u = v // 4, v % 4
            at = f * 32 + q * 8
            x = tails[at : at + 8]
            second.append(pltpu.roll(x, 8 - 2 * u, 0) if u else x)
        table = [first, second, second]
        for b in range(6, 3, -1):
            d = 1 << (b - 4)
            bit = ((shift >> b) & 1) == 1
            table = [
                [jnp.where(bit, rows_down(table[max(k - 1, 0)][v], table[k][v], d, s_io), table[k][v]) for v in range(NV)]
                for k in range(3)
            ]
        for b in range(3, -1, -1):
            d = 1 << b
            bit = ((shift >> b) & 1) == 1
            moved = []
            for k in range(3):
                row = []
                for v in range(NV):
                    if v >= d:
                        src = table[k][v - d]
                    else:
                        src = rows_down(table[max(k - 1, 0)][v - d + NV], table[k][v - d + NV], 1, s_io)
                    row.append(jnp.where(bit, src, table[k][v]))
                moved.append(row)
            table = moved
        picked = []
        for v in range(NV):
            x = [take_lanes(table[k][v], ranks[v]) for k in range(3)]
            picked.append(jnp.where(blocks[v] == 0, x[0], jnp.where(blocks[v] == 1, x[1], x[2])))
        values.append(picked)
    labels = [x & 16383 for x in keys]
    _, *values = network([labels] + values)
    for f in range(4):
        for v in range(NV):
            out_ref[f, v] = values[f][v]


def node_weights(coord):
    node = lax.broadcasted_iota(jnp.int32, (8, coord.shape[1]), 0)
    scale = jnp.full(node.shape, float(gll_scale[0]), jnp.float32)
    for a in range(1, 8):
        scale = jnp.where(node == a, float(gll_scale[a]), scale)
    factors = [jnp.where(node == b, 1.0, coord - float(gll_points[b])) for b in range(8)]
    while len(factors) > 1:
        factors = [factors[i] * factors[i + 1] for i in range(0, len(factors), 2)]
    return factors[0] * scale


def interpolate_kernel(got_ref, fields_ref, out_ref, tail_ref):
    sources = got_ref.shape[1]
    lane = lax.broadcasted_iota(jnp.int32, (sources // 4, 128), 1) >> 5
    ends = [got_ref[4, pl.ds(w, sources // 4, stride=4), :] for w in range(4)]
    tails = []
    for a in range(4):
        row = None
        for w in range(4):
            turn = (32 * (w - a)) % 128
            x = pltpu.roll(ends[w], turn, 1) if turn else ends[w]
            row = x if row is None else jnp.where(lane == w, x, row)
        tails.append(row)
    rows = sources + sources // 4
    element = lax.broadcasted_iota(jnp.int32, (128, 256), 0)

    def row_of(a, i):
        if i < sources:
            return got_ref[a, i : i + 1, :]
        return tails[a][i - sources : i - sources + 1, :]

    results = []
    for i in range(0, rows, 2):
        r, s, t, slot = [jnp.concatenate([row_of(a, i), row_of(a, i + 1)], axis=1) for a in range(4)]
        weight_r, weight_s, weight_t = node_weights(r), node_weights(s), node_weights(t)
        onehot = (element == slot.astype(jnp.int32)).astype(jnp.float32).astype(jnp.bfloat16)
        onehot = onehot.reshape(8, 16, 256)
        parts = []
        for c in range(8):
            w = jnp.broadcast_to(weight_t[c : c + 1], (16, 256)).astype(jnp.bfloat16)
            parts.append((onehot * w[None]).reshape(128, 256))
        picker = jnp.concatenate(parts, axis=0)
        along = jnp.dot(fields_ref[...], picker, preferred_element_type=jnp.float32)
        along = along.reshape(4, 8, 8, 256)
        along = jnp.sum(along * weight_r[None, :, None, :], axis=1)
        value = jnp.sum(along * weight_s[None], axis=1)
        for h in range(2):
            for f in range(4):
                piece = value[f : f + 1, 128 * h : 128 * h + 128]
                if i + h < sources:
                    out_ref[f, i + h : i + h + 1, :] = piece
                else:
                    tail_ref[f, i + h - sources : i + h - sources + 1, :] = piece
    for w in range(4):
        row = None
        for f in range(4):
            turn = (32 * (f - w)) % 128
            x = tail_ref[f, 0 : sources // 4, :]
            x = pltpu.roll(x, turn, 1) if turn else x
            row = x if row is None else jnp.where(lane == f, x, row)
        out_ref[4, pl.ds(w, sources // 4, stride=4), :] = row


def dispatch(rank, slot, coords):
    return pl.pallas_call(
        dispatch_kernel,
        out_shape=[
            jax.ShapeDtypeStruct((5, 128, 128), jnp.float32),
            jax.ShapeDtypeStruct((NV, 8, 128), jnp.int32),
            jax.ShapeDtypeStruct((2, 8, 128), jnp.int32),
        ],
        name="dispatch",
    )(rank, slot, coords)


def interpolate(got, table, chunk=32):
    return pl.pallas_call(
        interpolate_kernel,
        grid=(128 // chunk,),
        in_specs=[
            pl.BlockSpec((5, chunk, 128), lambda i: (0, i, 0)),
            pl.BlockSpec((256, 1024), lambda i: (0, 0)),
        ],
        out_specs=pl.BlockSpec((5, chunk, 128), lambda i: (0, i, 0)),
        out_shape=jax.ShapeDtypeStruct((5, 128, 128), jnp.float32),
        scratch_shapes=[pltpu.VMEM((4, 8, 128), jnp.float32)],
        name="interpolate",
    )(got, table)


def give_back(back, key, meta):
    return pl.pallas_call(
        return_kernel,
        out_shape=jax.ShapeDtypeStruct((4, NV, 8, 128), jnp.float32),
        name="give_back",
    )(back, key, meta)


def local(fields, coordinates, element_rank, element_slot):
    rank = element_rank.reshape(NV, 8, 128)
    slot = element_slot.reshape(NV, 8, 128)
    coords = coordinates.reshape(3, NV, 8, 128)
    table = fields.reshape(128, 256, 8).transpose(1, 2, 0).reshape(256, 1024)
    send, key, meta = dispatch(rank, slot, coords)
    got = lax.all_to_all(send, AXES, split_axis=1, concat_axis=1, tiled=True)
    values = interpolate(got, table)
    back = lax.all_to_all(values, AXES, split_axis=1, concat_axis=1, tiled=True)
    return give_back(back, key, meta).reshape(4, 16384)


def solution(mesh):
    placed = (P(AXES, None), P(None, AXES), P(AXES, None), P(AXES))
    return jax.shard_map(local, mesh=mesh, in_specs=placed, out_specs=P(None, AXES), check_vma=False)
```

```python
import jax
import jax.numpy as jnp
import numpy as np
from jax import lax
from jax.experimental import pallas as pl
from jax.experimental.pallas import tpu as pltpu
from jax.sharding import PartitionSpec as P

AXES = ("gx", "gy", "gz")
MESH = pl.DeviceIdType.MESH
CHUNK = 16
NV = 16

gll_points = np.array(
    [
        -1.0,
        -0.8717401485096066,
        -0.5917001814331423,
        -0.2092992179024789,
        0.2092992179024789,
        0.5917001814331423,
        0.8717401485096066,
        1.0,
    ]
)
gll_scale = np.array(
    [1.0 / np.prod([gll_points[a] - gll_points[b] for b in range(8) if b != a]) for a in range(8)]
)


def iotas():
    return lax.broadcasted_iota(jnp.int32, (8, 128), 0), lax.broadcasted_iota(jnp.int32, (8, 128), 1)


def partner(x, axis, d, bit):
    n = x.shape[axis]
    if 2 * d == n:
        return pltpu.roll(x, d, axis)
    if axis == 1:
        idx = lax.broadcasted_iota(jnp.int32, x.shape, 1) ^ d
        return jnp.take_along_axis(x, idx, axis=1)
    return jnp.where(bit, pltpu.roll(x, d, axis), pltpu.roll(x, n - d, axis))


def network(arrs):
    s_io, l_io = iotas()
    arrs = [list(a) for a in arrs]
    count = len(arrs)

    def bit_of(b):
        if b < 7:
            return ((s_io >> (b - 4)) & 1) == 1
        return ((l_io >> (b - 7)) & 1) == 1

    for k in range(1, 15):
        down = bit_of(k) if 4 <= k < 14 else None
        for j in range(k - 1, 3, -1):
            axis, d = (0, 1 << (j - 4)) if j < 7 else (1, 1 << (j - 7))
            upper = bit_of(j)
            flip = upper if down is None else jnp.logical_xor(upper, down)
            for v in range(NV):
                other = [partner(arrs[a][v], axis, d, upper) for a in range(count)]
                take = jnp.logical_xor(arrs[0][v] > other[0], flip)
                for a in range(count):
                    arrs[a][v] = jnp.where(take, other[a], arrs[a][v])
        for j in range(min(k, 4) - 1, -1, -1):
            d = 1 << j
            for v in range(NV):
                if v & d:
                    continue
                w = v | d
                if k < 4 and (v >> k) & 1:
                    swap = arrs[0][v] < arrs[0][w]
                else:
                    swap = arrs[0][v] > arrs[0][w]
                if down is not None:
                    swap = jnp.logical_xor(swap, down)
                for a in range(count):
                    x, y = arrs[a][v], arrs[a][w]
                    arrs[a][v] = jnp.where(swap, y, x)
                    arrs[a][w] = jnp.where(swap, x, y)
    return arrs


def take_lanes(x, idx):
    return jnp.take_along_axis(x, idx, axis=1)


def rows_up(low, high, d, s_io):
    return jnp.where(s_io < 8 - d, pltpu.roll(low, 8 - d, 0), pltpu.roll(high, 8 - d, 0))


def rows_down(low, high, d, s_io):
    return jnp.where(s_io >= d, pltpu.roll(high, d, 0), pltpu.roll(low, d, 0))


def dispatch_kernel(rank_ref, slot_ref, coord_ref, send_ref, key_ref, meta_ref):
    s_io, l_io = iotas()
    keys = []
    for v in range(NV):
        label = l_io * 128 + s_io * 16 + v
        keys.append(rank_ref[v] * (1 << 21) + slot_ref[v] * (1 << 14) + label)
    coords = [[coord_ref[c, v] for v in range(NV)] for c in range(3)]
    keys, *coords = network([keys] + coords)
    for v in range(NV):
        key_ref[v] = keys[v]
    last = (keys[NV - 1][7:8, :] >> 21).astype(jnp.float32)
    last = jnp.broadcast_to(last, (128, 128)).T
    lanes = lax.broadcasted_iota(jnp.int32, (128, 128), 1).astype(jnp.float32)
    column = jnp.sum((last < lanes).astype(jnp.float32), axis=0, keepdims=True)
    column = jnp.broadcast_to(column, (8, 128)).astype(jnp.int32)
    columns = [jnp.minimum(column + k, 127) for k in range(3)]
    spread = [[take_lanes(keys[v], columns[k]) for v in range(NV)] for k in range(3)]
    below = jnp.zeros((8, 128), jnp.float32)
    for v in range(NV):
        below = below + ((spread[0][v] >> 21) < l_io).astype(jnp.float32)
    shift = jnp.broadcast_to(jnp.sum(below, axis=0, keepdims=True), (8, 128)).astype(jnp.int32)
    meta_ref[0] = column
    meta_ref[1] = shift

    tails = []
    for a in range(4):
        if a == 3:
            table = [[((x >> 14) & 127).astype(jnp.float32) for x in block] for block in spread]
        else:
            table = [[take_lanes(coords[a][v], columns[k]) for v in range(NV)] for k in range(3)]
        for b in range(4):
            d = 1 << b
            bit = ((shift >> b) & 1) == 1
            moved = []
            for k in range(3):
                row = []
                for v in range(NV):
                    if v + d < NV:
                        src = table[k][v + d]
                    else:
                        src = rows_up(table[k][v + d - NV], table[min(k + 1, 2)][v + d - NV], 1, s_io)
                    row.append(jnp.where(bit, src, table[k][v]))
                moved.append(row)
            table = moved
        for b in range(4, 7):
            d = 1 << (b - 4)
            bit = ((shift >> b) & 1) == 1
            moved = [
                [
                    jnp.where(bit, rows_up(table[k][v], table[min(k + 1, len(table) - 1)][v], d, s_io), table[k][v])
                    for v in range(NV)
                ]
                for k in range(2)
            ]
            table = moved
        send_ref[a] = jnp.concatenate(table[0], axis=0).T
        for q in range(4):
            tail = table[1][4 * q]
            for u in range(1, 4):
                tail = jnp.where(s_io >= 2 * u, pltpu.roll(table[1][4 * q + u], 2 * u, 0), tail)
            tails.append(tail)
    send_ref[4] = jnp.concatenate(tails, axis=0).T


def return_kernel(back_ref, key_ref, meta_ref, out_ref):
    s_io, l_io = iotas()
    column, shift = meta_ref[0], meta_ref[1]
    keys = [key_ref[v] for v in range(NV)]
    ranks = [x >> 21 for x in keys]
    blocks = [l_io - take_lanes(column, x) for x in ranks]
    tails = back_ref[4].T
    values = []
    for f in range(4):
        main = back_ref[f].T
        first = [main[8 * v : 8 * v + 8] for v in range(NV)]
        second = []
        for v in range(NV):
            q, u = v // 4, v % 4
            at = f * 32 + q * 8
            x = tails[at : at + 8]
            second.append(pltpu.roll(x, 8 - 2 * u, 0) if u else x)
        table = [first, second, second]
        for b in range(6, 3, -1):
            d = 1 << (b - 4)
            bit = ((shift >> b) & 1) == 1
            table = [
                [jnp.where(bit, rows_down(table[max(k - 1, 0)][v], table[k][v], d, s_io), table[k][v]) for v in range(NV)]
                for k in range(3)
            ]
        for b in range(3, -1, -1):
            d = 1 << b
            bit = ((shift >> b) & 1) == 1
            moved = []
            for k in range(3):
                row = []
                for v in range(NV):
                    if v >= d:
                        src = table[k][v - d]
                    else:
                        src = rows_down(table[max(k - 1, 0)][v - d + NV], table[k][v - d + NV], 1, s_io)
                    row.append(jnp.where(bit, src, table[k][v]))
                moved.append(row)
            table = moved
        picked = []
        for v in range(NV):
            x = [take_lanes(table[k][v], ranks[v]) for k in range(3)]
            picked.append(jnp.where(blocks[v] == 0, x[0], jnp.where(blocks[v] == 1, x[1], x[2])))
        values.append(picked)
    labels = [x & 16383 for x in keys]
    _, *values = network([labels] + values)
    for f in range(4):
        for v in range(NV):
            out_ref[f, v] = values[f][v]


def node_weights(coord):
    node = lax.broadcasted_iota(jnp.int32, (8, coord.shape[1]), 0)
    scale = jnp.full(node.shape, float(gll_scale[0]), jnp.float32)
    for a in range(1, 8):
        scale = jnp.where(node == a, float(gll_scale[a]), scale)
    factors = [jnp.where(node == b, 1.0, coord - float(gll_points[b])) for b in range(8)]
    while len(factors) > 1:
        factors = [factors[i] * factors[i + 1] for i in range(0, len(factors), 2)]
    return factors[0] * scale


def offsets(slot):
    return (slot // 4) % 4, slot % 4, slot // 16


def exchange_kernel(send, table, back, got, vals, send_sem, got_sems, value_sem, back_sem):
    gx, gy, gz = (lax.axis_index(name) for name in AXES)
    me = gx * 32 + gy * 8 + gz

    def ahead(slot):
        dx, dy, dz = offsets(slot)
        return (gx + dx) % 4, (gy + dy) % 4, (gz + dz) % 8

    def behind(slot):
        dx, dy, dz = offsets(slot)
        return (gx + 4 - dx) % 4, (gy + 4 - dy) % 4, (gz + 8 - dz) % 8

    def number(where):
        return where[0] * 32 + where[1] * 8 + where[2]

    barrier = pltpu.get_barrier_semaphore()

    def greet(slot, carry):
        pl.semaphore_signal(barrier, inc=1, device_id=ahead(slot), device_id_type=MESH)
        return carry

    lax.fori_loop(1, 128, greet, 0)
    pl.semaphore_wait(barrier, 127)

    pltpu.make_async_copy(send.at[:, me], got.at[:, 0], got_sems.at[0]).start()

    def ship(slot, carry):
        where = ahead(slot)
        pltpu.make_async_remote_copy(
            src_ref=send.at[:, number(where)],
            dst_ref=got.at[:, slot],
            send_sem=send_sem,
            recv_sem=got_sems.at[slot // CHUNK],
            device_id=where,
            device_id_type=MESH,
        ).start()
        return carry

    lax.fori_loop(1, 128, ship, 0)

    lane = lax.broadcasted_iota(jnp.int32, (1, 128), 1) >> 5
    element = lax.broadcasted_iota(jnp.int32, (128, 256), 0)

    def work(chunk, carry):
        base = chunk * CHUNK
        block = got.at[:, pl.ds(base, CHUNK)]
        pltpu.make_async_copy(block, block, got_sems.at[chunk]).wait()
        rows = [[got[a, base + i] for a in range(4)] for i in range(CHUNK)]
        for i in range(CHUNK // 4):
            ends = [got[4, base + 4 * i + w] for w in range(4)]
            tail = []
            for a in range(4):
                row = None
                for w in range(4):
                    turn = (32 * (w - a)) % 128
                    x = pltpu.roll(ends[w], turn, 1) if turn else ends[w]
                    row = x if row is None else jnp.where(lane == w, x, row)
                tail.append(row)
            rows.append(tail)
        found = []
        for i in range(0, len(rows), 2):
            r, s, t, slot = [jnp.concatenate([rows[i][a], rows[i + 1][a]], axis=1) for a in range(4)]
            weight_r, weight_s, weight_t = node_weights(r), node_weights(s), node_weights(t)
            onehot = (element == slot.astype(jnp.int32)).astype(jnp.float32).astype(jnp.bfloat16)
            onehot = onehot.reshape(8, 16, 256)
            parts = []
            for c in range(8):
                w = jnp.broadcast_to(weight_t[c : c + 1], (16, 256)).astype(jnp.bfloat16)
                parts.append((onehot * w[None]).reshape(128, 256))
            picker = jnp.concatenate(parts, axis=0)
            along = jnp.dot(table[...], picker, preferred_element_type=jnp.float32)
            along = along.reshape(4, 8, 8, 256)
            along = jnp.sum(along * weight_r[None, :, None, :], axis=1)
            value = jnp.sum(along * weight_s[None], axis=1)
            for h in range(2):
                pieces = [value[f : f + 1, 128 * h : 128 * h + 128] for f in range(4)]
                if i + h < CHUNK:
                    for f in range(4):
                        vals[f, base + i + h] = pieces[f]
                else:
                    found.append(pieces)
        for i in range(CHUNK // 4):
            for w in range(4):
                row = None
                for f in range(4):
                    turn = (32 * (f - w)) % 128
                    x = pltpu.roll(found[i][f], turn, 1) if turn else found[i][f]
                    row = x if row is None else jnp.where(lane == f, x, row)
                vals[4, base + 4 * i + w] = row

        def answer(slot, inner):
            where = behind(slot)

            @pl.when(slot == 0)
            def _():
                pltpu.make_async_copy(vals.at[:, 0], back.at[:, me], back_sem).start()

            @pl.when(slot > 0)
            def _():
                pltpu.make_async_remote_copy(
                    src_ref=vals.at[:, slot],
                    dst_ref=back.at[:, me],
                    send_sem=value_sem,
                    recv_sem=back_sem,
                    device_id=where,
                    device_id_type=MESH,
                ).start()

            return inner

        lax.fori_loop(base, base + CHUNK, answer, 0)
        return carry

    lax.fori_loop(0, 128 // CHUNK, work, 0)
    sent = send.at[:, pl.ds(0, 127)]
    pltpu.make_async_copy(sent, sent, send_sem).wait()
    told = vals.at[:, pl.ds(0, 127)]
    pltpu.make_async_copy(told, told, value_sem).wait()
    pltpu.make_async_copy(back, back, back_sem).wait()


def dispatch(rank, slot, coords):
    return pl.pallas_call(
        dispatch_kernel,
        out_shape=[
            jax.ShapeDtypeStruct((5, 128, 128), jnp.float32),
            jax.ShapeDtypeStruct((NV, 8, 128), jnp.int32),
            jax.ShapeDtypeStruct((2, 8, 128), jnp.int32),
        ],
        name="dispatch",
    )(rank, slot, coords)


def exchange(send, table):
    return pl.pallas_call(
        exchange_kernel,
        in_specs=[pl.BlockSpec(memory_space=pltpu.VMEM)] * 2,
        out_specs=pl.BlockSpec(memory_space=pltpu.VMEM),
        out_shape=jax.ShapeDtypeStruct((5, 128, 1, 128), jnp.float32),
        scratch_shapes=[
            pltpu.VMEM((5, 128, 1, 128), jnp.float32),
            pltpu.VMEM((5, 128, 1, 128), jnp.float32),
            pltpu.SemaphoreType.DMA,
            pltpu.SemaphoreType.DMA((128 // CHUNK,)),
            pltpu.SemaphoreType.DMA,
            pltpu.SemaphoreType.DMA,
        ],
        compiler_params=pltpu.CompilerParams(collective_id=0, has_side_effects=True),
        name="exchange",
    )(send, table)


def give_back(back, key, meta):
    return pl.pallas_call(
        return_kernel,
        out_shape=jax.ShapeDtypeStruct((4, NV, 8, 128), jnp.float32),
        name="give_back",
    )(back, key, meta)


def local(fields, coordinates, element_rank, element_slot):
    rank = element_rank.reshape(NV, 8, 128)
    slot = element_slot.reshape(NV, 8, 128)
    coords = coordinates.reshape(3, NV, 8, 128)
    table = fields.reshape(128, 256, 8).transpose(1, 2, 0).reshape(256, 1024)
    send, key, meta = dispatch(rank, slot, coords)
    back = exchange(send.reshape(5, 128, 1, 128), table).reshape(5, 128, 128)
    return give_back(back, key, meta).reshape(4, 16384)


def solution(mesh):
    placed = (P(AXES, None), P(None, AXES), P(AXES, None), P(AXES))
    return jax.shard_map(local, mesh=mesh, in_specs=placed, out_specs=P(None, AXES), check_vma=False)
```

```python
import functools

import jax
import jax.numpy as jnp
import numpy as np
from jax import lax
from jax.experimental import pallas as pl
from jax.experimental.pallas import tpu as pltpu
from jax.sharding import PartitionSpec as P

AXES = ("gx", "gy", "gz")
LOGICAL = pl.DeviceIdType.LOGICAL
CHUNK = 16
LEVELS = (1 << 21) - 1
NV = 16

gll_points = np.array(
    [
        -1.0,
        -0.8717401485096066,
        -0.5917001814331423,
        -0.2092992179024789,
        0.2092992179024789,
        0.5917001814331423,
        0.8717401485096066,
        1.0,
    ]
)
gll_scale = np.array(
    [1.0 / np.prod([gll_points[a] - gll_points[b] for b in range(8) if b != a]) for a in range(8)]
)


def iotas():
    return lax.broadcasted_iota(jnp.int32, (8, 128), 0), lax.broadcasted_iota(jnp.int32, (8, 128), 1)


def partner(x, axis, d, bit):
    n = x.shape[axis]
    if 2 * d == n:
        return pltpu.roll(x, d, axis)
    if axis == 1:
        idx = lax.broadcasted_iota(jnp.int32, x.shape, 1) ^ d
        return jnp.take_along_axis(x, idx, axis=1)
    return jnp.where(bit, pltpu.roll(x, d, axis), pltpu.roll(x, n - d, axis))


def network(arrs):
    s_io, l_io = iotas()
    arrs = [list(a) for a in arrs]
    count = len(arrs)

    def bit_of(b):
        if b < 7:
            return ((s_io >> (b - 4)) & 1) == 1
        return ((l_io >> (b - 7)) & 1) == 1

    for k in range(1, 15):
        down = bit_of(k) if 4 <= k < 14 else None
        for j in range(k - 1, 3, -1):
            axis, d = (0, 1 << (j - 4)) if j < 7 else (1, 1 << (j - 7))
            upper = bit_of(j)
            flip = upper if down is None else jnp.logical_xor(upper, down)
            for v in range(NV):
                other = [partner(arrs[a][v], axis, d, upper) for a in range(count)]
                take = jnp.logical_xor(arrs[0][v] > other[0], flip)
                for a in range(count):
                    arrs[a][v] = jnp.where(take, other[a], arrs[a][v])
        for j in range(min(k, 4) - 1, -1, -1):
            d = 1 << j
            for v in range(NV):
                if v & d:
                    continue
                w = v | d
                if k < 4 and (v >> k) & 1:
                    swap = arrs[0][v] < arrs[0][w]
                else:
                    swap = arrs[0][v] > arrs[0][w]
                if down is not None:
                    swap = jnp.logical_xor(swap, down)
                for a in range(count):
                    x, y = arrs[a][v], arrs[a][w]
                    arrs[a][v] = jnp.where(swap, y, x)
                    arrs[a][w] = jnp.where(swap, x, y)
    return arrs


def take_lanes(x, idx):
    return jnp.take_along_axis(x, idx, axis=1)


def rows_up(low, high, d, s_io):
    return jnp.where(s_io < 8 - d, pltpu.roll(low, 8 - d, 0), pltpu.roll(high, 8 - d, 0))


def rows_down(low, high, d, s_io):
    return jnp.where(s_io >= d, pltpu.roll(high, d, 0), pltpu.roll(low, d, 0))


def hold(x):
    return ((x + 1.0) * (LEVELS / 2) + 0.5).astype(jnp.int32)


def release(q):
    return q.astype(jnp.float32) * (2 / LEVELS) - 1.0


def right(x, count):
    return lax.shift_right_logical(x, jnp.full(x.shape, count, jnp.int32))


def dispatch_steps(rank_ref, slot_ref, coord_ref, send_ref, key_ref, meta_ref):
    s_io, l_io = iotas()
    words = [[], [], []]
    for v in range(NV):
        label = l_io * 128 + s_io * 16 + v
        r, s, t = [hold(coord_ref[8 * v : 8 * v + 8, c, :]) for c in range(3)]
        words[0].append(rank_ref[v] * (1 << 21) + slot_ref[v] * (1 << 14) + label)
        words[1].append((r << 11) | (t >> 10))
        words[2].append((s << 11) | (t & 1023))
    words = network(words)
    keys = words[0]
    for v in range(NV):
        key_ref[v] = keys[v]
    last = (keys[NV - 1][7:8, :] >> 21).astype(jnp.float32)
    last = jnp.broadcast_to(last, (128, 128)).T
    lanes = lax.broadcasted_iota(jnp.int32, (128, 128), 1).astype(jnp.float32)
    column = jnp.sum((last < lanes).astype(jnp.float32), axis=0, keepdims=True)
    column = jnp.broadcast_to(column, (8, 128)).astype(jnp.int32)
    columns = [jnp.minimum(column + k, 127) for k in range(3)]
    spread = [[take_lanes(keys[v], columns[k]) for v in range(NV)] for k in range(3)]
    below = jnp.zeros((8, 128), jnp.float32)
    for v in range(NV):
        below = below + ((spread[0][v] >> 21) < l_io).astype(jnp.float32)
    shift = jnp.broadcast_to(jnp.sum(below, axis=0, keepdims=True), (8, 128)).astype(jnp.int32)
    meta_ref[0] = column
    meta_ref[1] = shift

    moved_words = []
    for a in range(3):
        table = spread if a == 0 else [[take_lanes(words[a][v], columns[k]) for v in range(NV)] for k in range(3)]
        for b in range(4):
            d = 1 << b
            bit = ((shift >> b) & 1) == 1
            moved = []
            for k in range(3):
                row = []
                for v in range(NV):
                    if v + d < NV:
                        src = table[k][v + d]
                    else:
                        src = rows_up(table[k][v + d - NV], table[min(k + 1, 2)][v + d - NV], 1, s_io)
                    row.append(jnp.where(bit, src, table[k][v]))
                moved.append(row)
            table = moved
        for b in range(4, 7):
            d = 1 << (b - 4)
            bit = ((shift >> b) & 1) == 1
            table = [
                [
                    jnp.where(bit, rows_up(table[k][v], table[min(k + 1, len(table) - 1)][v], d, s_io), table[k][v])
                    for v in range(NV)
                ]
                for k in range(2)
            ]
        rows = list(table[0])
        for q in range(4):
            tail = table[1][4 * q]
            for u in range(1, 4):
                tail = jnp.where(s_io >= 2 * u, pltpu.roll(table[1][4 * q + u], 2 * u, 0), tail)
            rows.append(tail)
        moved_words.append(rows)
    key, first, second = moved_words
    split = [
        [release(right(x, 11)) for x in first],
        [release(right(x, 11)) for x in second],
        [release(((x & 2047) << 10) | (y & 1023)) for x, y in zip(first, second)],
        [((x >> 14) & 127).astype(jnp.float32) for x in key],
    ]
    for a in range(4):
        send_ref[a] = jnp.concatenate(split[a][:NV], axis=0).T
    send_ref[4] = jnp.concatenate([x for a in range(4) for x in split[a][NV:]], axis=0).T


def return_kernel(back_ref, key_ref, meta_ref, out_ref):
    s_io, l_io = iotas()
    column, shift = meta_ref[0], meta_ref[1]
    keys = [key_ref[v] for v in range(NV)]
    ranks = [x >> 21 for x in keys]
    blocks = [l_io - take_lanes(column, x) for x in ranks]
    tails = back_ref[4].T
    values = []
    for f in range(4):
        main = back_ref[f].T
        first = [main[8 * v : 8 * v + 8] for v in range(NV)]
        second = []
        for v in range(NV):
            q, u = v // 4, v % 4
            at = f * 32 + q * 8
            x = tails[at : at + 8]
            second.append(pltpu.roll(x, 8 - 2 * u, 0) if u else x)
        table = [first, second, second]
        for b in range(6, 3, -1):
            d = 1 << (b - 4)
            bit = ((shift >> b) & 1) == 1
            table = [
                [jnp.where(bit, rows_down(table[max(k - 1, 0)][v], table[k][v], d, s_io), table[k][v]) for v in range(NV)]
                for k in range(3)
            ]
        for b in range(3, -1, -1):
            d = 1 << b
            bit = ((shift >> b) & 1) == 1
            moved = []
            for k in range(3):
                row = []
                for v in range(NV):
                    if v >= d:
                        src = table[k][v - d]
                    else:
                        src = rows_down(table[max(k - 1, 0)][v - d + NV], table[k][v - d + NV], 1, s_io)
                    row.append(jnp.where(bit, src, table[k][v]))
                moved.append(row)
            table = moved
        picked = []
        for v in range(NV):
            x = [take_lanes(table[k][v], ranks[v]) for k in range(3)]
            picked.append(jnp.where(blocks[v] == 0, x[0], jnp.where(blocks[v] == 1, x[1], x[2])))
        values.append(picked)
    largest = functools.reduce(jnp.maximum, [jnp.abs(x) for picked in values for x in picked])
    largest = jnp.maximum(jnp.max(jnp.max(largest, axis=0, keepdims=True), axis=1, keepdims=True), 1e-30)
    grow = jnp.broadcast_to(524287.0 / largest, (8, 128))
    shrink = jnp.broadcast_to(largest / 524287.0, (8, 128))
    words = [[], [], []]
    for v in range(NV):
        q = [(values[f][v] * grow + 524288.5).astype(jnp.int32) for f in range(4)]
        low = ((q[0] & 15) << 12) | ((q[1] & 15) << 8) | ((q[2] & 15) << 4) | (q[3] & 15)
        words[0].append(((keys[v] & 16383) << 16) | low)
        words[1].append(((q[0] >> 4) << 16) | (q[1] >> 4))
        words[2].append(((q[2] >> 4) << 16) | (q[3] >> 4))
    words = network(words)
    for v in range(NV):
        low, first, second = [words[a][v] for a in range(3)]
        q = [
            (right(first, 16) << 4) | ((low >> 12) & 15),
            ((first & 65535) << 4) | ((low >> 8) & 15),
            (right(second, 16) << 4) | ((low >> 4) & 15),
            ((second & 65535) << 4) | (low & 15),
        ]
        for f in range(4):
            out_ref[8 * v : 8 * v + 8, f, :] = (q[f] - 524288).astype(jnp.float32) * shrink


def node_weights(coord):
    node = lax.broadcasted_iota(jnp.int32, (8, coord.shape[1]), 0)
    scale = jnp.full(node.shape, float(gll_scale[0]), jnp.float32)
    for a in range(1, 8):
        scale = jnp.where(node == a, float(gll_scale[a]), scale)
    factors = [jnp.where(node == b, 1.0, coord - float(gll_points[b])) for b in range(8)]
    while len(factors) > 1:
        factors = [factors[i] * factors[i + 1] for i in range(0, len(factors), 2)]
    return factors[0] * scale


def exchange_kernel(
    rank_ref, slot_ref, coord_ref, table, back, key_ref, meta_ref, send, got, vals, send_sem, got_sems, value_sem, back_sem
):
    gx, gy, gz = (lax.axis_index(name) for name in AXES)
    me = gx * 32 + gy * 8 + gz

    def ahead(dx, dy, dz):
        return ((gx + dx) % 4) * 32 + ((gy + dy) % 4) * 8 + (gz + dz) % 8

    def behind(dx, dy, dz):
        return ((gx + 4 - dx) % 4) * 32 + ((gy + 4 - dy) % 4) * 8 + (gz + 8 - dz) % 8

    def steps(chunk, half):
        dx = chunk // 2
        return dx, ((chunk + dx) % 2) * 2 + half

    targets = [ahead(*steps(slot // 16, (slot // 8) % 2), slot % 8) for slot in range(128)]
    barrier = pltpu.get_barrier_semaphore()
    for slot in range(1, 128):
        pl.semaphore_signal(barrier, inc=1, device_id=targets[slot], device_id_type=LOGICAL)

    dispatch_steps(rank_ref, slot_ref, coord_ref, send, key_ref, meta_ref)

    pl.semaphore_wait(barrier, 127)
    pltpu.make_async_copy(send.at[:, pl.ds(me, 1)], got.at[:, pl.ds(0, 1)], got_sems.at[0]).start()
    for slot in range(1, 128):
        pltpu.make_async_remote_copy(
            src_ref=send.at[:, pl.ds(targets[slot], 1)],
            dst_ref=got.at[:, pl.ds(slot, 1)],
            send_sem=send_sem,
            recv_sem=got_sems.at[slot // CHUNK],
            device_id=targets[slot],
            device_id_type=LOGICAL,
        ).start()

    lane = lax.broadcasted_iota(jnp.int32, (1, 128), 1) >> 5
    element = lax.broadcasted_iota(jnp.int32, (128, 256), 0)

    def work(chunk, carry):
        base = chunk * CHUNK
        block = got.at[:, pl.ds(base, CHUNK)]
        pltpu.make_async_copy(block, block, got_sems.at[chunk]).wait()
        rows = [[got[a, pl.ds(base + i, 1), :] for a in range(4)] for i in range(CHUNK)]
        for i in range(CHUNK // 4):
            ends = [got[4, pl.ds(base + 4 * i + w, 1), :] for w in range(4)]
            tail = []
            for a in range(4):
                row = None
                for w in range(4):
                    turn = (32 * (w - a)) % 128
                    x = pltpu.roll(ends[w], turn, 1) if turn else ends[w]
                    row = x if row is None else jnp.where(lane == w, x, row)
                tail.append(row)
            rows.append(tail)
        found = []
        for i in range(0, len(rows), 2):
            r, s, t, slot = [jnp.concatenate([rows[i][a], rows[i + 1][a]], axis=1) for a in range(4)]
            weight_r, weight_s, weight_t = node_weights(r), node_weights(s), node_weights(t)
            onehot = (element == slot.astype(jnp.int32)).astype(jnp.float32).astype(jnp.bfloat16)
            onehot = onehot.reshape(8, 16, 256)
            parts = []
            for c in range(8):
                w = jnp.broadcast_to(weight_t[c : c + 1], (16, 256)).astype(jnp.bfloat16)
                parts.append((onehot * w[None]).reshape(128, 256))
            picker = jnp.concatenate(parts, axis=0)
            along = jnp.dot(table[...], picker, preferred_element_type=jnp.float32)
            along = along.reshape(4, 8, 8, 256)
            along = jnp.sum(along * weight_r[None, :, None, :], axis=1)
            value = jnp.sum(along * weight_s[None], axis=1)
            for h in range(2):
                pieces = [value[f : f + 1, 128 * h : 128 * h + 128] for f in range(4)]
                if i + h < CHUNK:
                    for f in range(4):
                        vals[f, pl.ds(base + i + h, 1), :] = pieces[f]
                else:
                    found.append(pieces)
        for i in range(CHUNK // 4):
            for w in range(4):
                row = None
                for f in range(4):
                    turn = (32 * (f - w)) % 128
                    x = pltpu.roll(found[i][f], turn, 1) if turn else found[i][f]
                    row = x if row is None else jnp.where(lane == f, x, row)
                vals[4, pl.ds(base + 4 * i + w, 1), :] = row

        for i in range(CHUNK):
            dx, dy = steps(base // 16, (i // 8) % 2)
            where = behind(dx, dy, i % 8)

            def local_answer():
                pltpu.make_async_copy(vals.at[:, pl.ds(0, 1)], back.at[:, pl.ds(me, 1)], back_sem).start()

            def answer():
                pltpu.make_async_remote_copy(
                    src_ref=vals.at[:, pl.ds(base + i, 1)],
                    dst_ref=back.at[:, pl.ds(me, 1)],
                    send_sem=value_sem,
                    recv_sem=back_sem,
                    device_id=where,
                    device_id_type=LOGICAL,
                ).start()

            if i == 0:
                pl.when(chunk == 0)(local_answer)
                pl.when(chunk > 0)(answer)
            else:
                answer()
        return carry

    lax.fori_loop(0, 128 // CHUNK, work, 0)
    sent = send.at[:, pl.ds(0, 127)]
    pltpu.make_async_copy(sent, sent, send_sem).wait()
    told = vals.at[:, pl.ds(0, 127)]
    pltpu.make_async_copy(told, told, value_sem).wait()
    pltpu.make_async_copy(back, back, back_sem).wait()


def exchange(rank, slot, coords, table):
    return pl.pallas_call(
        exchange_kernel,
        in_specs=[pl.BlockSpec(memory_space=pltpu.VMEM)] * 4,
        out_specs=[pl.BlockSpec(memory_space=pltpu.VMEM)] * 3,
        out_shape=[
            jax.ShapeDtypeStruct((5, 128, 128), jnp.float32),
            jax.ShapeDtypeStruct((NV, 8, 128), jnp.int32),
            jax.ShapeDtypeStruct((2, 8, 128), jnp.int32),
        ],
        scratch_shapes=[
            pltpu.VMEM((5, 128, 128), jnp.float32),
            pltpu.VMEM((5, 128, 128), jnp.float32),
            pltpu.VMEM((5, 128, 128), jnp.float32),
            pltpu.SemaphoreType.DMA,
            pltpu.SemaphoreType.DMA((128 // CHUNK,)),
            pltpu.SemaphoreType.DMA,
            pltpu.SemaphoreType.DMA,
        ],
        compiler_params=pltpu.CompilerParams(collective_id=0, has_side_effects=True),
        name="exchange",
    )(rank, slot, coords, table)


def give_back(back, key, meta):
    return pl.pallas_call(
        return_kernel,
        out_shape=jax.ShapeDtypeStruct((128, 4, 128), jnp.float32),
        name="give_back",
    )(back, key, meta)


def local(fields, coordinates, element_rank, element_slot):
    rank = element_rank.reshape(NV, 8, 128)
    slot = element_slot.reshape(NV, 8, 128)
    coords = coordinates.reshape(3, 128, 128).transpose(1, 0, 2)
    table = fields.reshape(128, 256, 8).transpose(1, 2, 0).reshape(256, 1024)
    back, key, meta = exchange(rank, slot, coords, table)
    return give_back(back, key, meta).transpose(1, 0, 2).reshape(4, 16384)


def solution(mesh):
    placed = (P(AXES, None), P(None, AXES), P(AXES, None), P(AXES))
    return jax.shard_map(local, mesh=mesh, in_specs=placed, out_specs=P(None, AXES), check_vma=False)
```

```python
import functools

import jax
import jax.numpy as jnp
import numpy as np
from jax import lax
from jax.experimental import pallas as pl
from jax.experimental.pallas import tpu as pltpu
from jax.sharding import PartitionSpec as P

AXES = ("gx", "gy", "gz")
LOGICAL = pl.DeviceIdType.LOGICAL
LEVELS = (1 << 21) - 1
NV = 16

gll_points = np.array(
    [
        -1.0,
        -0.8717401485096066,
        -0.5917001814331423,
        -0.2092992179024789,
        0.2092992179024789,
        0.5917001814331423,
        0.8717401485096066,
        1.0,
    ]
)
gll_scale = np.array(
    [1.0 / np.prod([gll_points[a] - gll_points[b] for b in range(8) if b != a]) for a in range(8)]
)


def iotas():
    return lax.broadcasted_iota(jnp.int32, (8, 128), 0), lax.broadcasted_iota(jnp.int32, (8, 128), 1)


def partner(x, axis, d, bit):
    n = x.shape[axis]
    if 2 * d == n:
        return pltpu.roll(x, d, axis)
    if axis == 1:
        idx = lax.broadcasted_iota(jnp.int32, x.shape, 1) ^ d
        return jnp.take_along_axis(x, idx, axis=1)
    return jnp.where(bit, pltpu.roll(x, d, axis), pltpu.roll(x, n - d, axis))


def network(arrs):
    s_io, l_io = iotas()
    arrs = [list(a) for a in arrs]
    count = len(arrs)

    def bit_of(b):
        if b < 7:
            return ((s_io >> (b - 4)) & 1) == 1
        return ((l_io >> (b - 7)) & 1) == 1

    for k in range(1, 15):
        down = bit_of(k) if 4 <= k < 14 else None
        for j in range(k - 1, 3, -1):
            axis, d = (0, 1 << (j - 4)) if j < 7 else (1, 1 << (j - 7))
            upper = bit_of(j)
            flip = upper if down is None else jnp.logical_xor(upper, down)
            for v in range(NV):
                other = [partner(arrs[a][v], axis, d, upper) for a in range(count)]
                take = jnp.logical_xor(arrs[0][v] > other[0], flip)
                for a in range(count):
                    arrs[a][v] = jnp.where(take, other[a], arrs[a][v])
        for j in range(min(k, 4) - 1, -1, -1):
            d = 1 << j
            for v in range(NV):
                if v & d:
                    continue
                w = v | d
                if k < 4 and (v >> k) & 1:
                    swap = arrs[0][v] < arrs[0][w]
                else:
                    swap = arrs[0][v] > arrs[0][w]
                if down is not None:
                    swap = jnp.logical_xor(swap, down)
                for a in range(count):
                    x, y = arrs[a][v], arrs[a][w]
                    arrs[a][v] = jnp.where(swap, y, x)
                    arrs[a][w] = jnp.where(swap, x, y)
    return arrs


def take_lanes(x, idx):
    return jnp.take_along_axis(x, idx, axis=1)


def rows_up(low, high, d, s_io):
    return jnp.where(s_io < 8 - d, pltpu.roll(low, 8 - d, 0), pltpu.roll(high, 8 - d, 0))


def rows_down(low, high, d, s_io):
    return jnp.where(s_io >= d, pltpu.roll(high, d, 0), pltpu.roll(low, d, 0))


def hold(x):
    return ((x + 1.0) * (LEVELS / 2) + 0.5).astype(jnp.int32)


def release(q):
    return q.astype(jnp.float32) * (2 / LEVELS) - 1.0


def right(x, count):
    return lax.shift_right_logical(x, jnp.full(x.shape, count, jnp.int32))


def dispatch_steps(rank_ref, slot_ref, coord_ref, send_ref, key_ref, meta_ref):
    s_io, l_io = iotas()
    words = [[], [], []]
    for v in range(NV):
        label = l_io * 128 + s_io * 16 + v
        r, s, t = [hold(coord_ref[8 * v : 8 * v + 8, c, :]) for c in range(3)]
        words[0].append(rank_ref[v] * (1 << 21) + slot_ref[v] * (1 << 14) + label)
        words[1].append((r << 11) | (t >> 10))
        words[2].append((s << 11) | (t & 1023))
    words = network(words)
    keys = words[0]
    for v in range(NV):
        key_ref[v] = keys[v]
    last = (keys[NV - 1][7:8, :] >> 21).astype(jnp.float32)
    last = jnp.broadcast_to(last, (128, 128)).T
    lanes = lax.broadcasted_iota(jnp.int32, (128, 128), 1).astype(jnp.float32)
    column = jnp.sum((last < lanes).astype(jnp.float32), axis=0, keepdims=True)
    column = jnp.broadcast_to(column, (8, 128)).astype(jnp.int32)
    columns = [jnp.minimum(column + k, 127) for k in range(3)]
    spread = [[take_lanes(keys[v], columns[k]) for v in range(NV)] for k in range(3)]
    below = jnp.zeros((8, 128), jnp.float32)
    for v in range(NV):
        below = below + ((spread[0][v] >> 21) < l_io).astype(jnp.float32)
    shift = jnp.broadcast_to(jnp.sum(below, axis=0, keepdims=True), (8, 128)).astype(jnp.int32)
    meta_ref[0] = column
    meta_ref[1] = shift

    moved_words = []
    for a in range(3):
        table = spread if a == 0 else [[take_lanes(words[a][v], columns[k]) for v in range(NV)] for k in range(3)]
        for b in range(4):
            d = 1 << b
            bit = ((shift >> b) & 1) == 1
            moved = []
            for k in range(3):
                row = []
                for v in range(NV):
                    if v + d < NV:
                        src = table[k][v + d]
                    else:
                        src = rows_up(table[k][v + d - NV], table[min(k + 1, 2)][v + d - NV], 1, s_io)
                    row.append(jnp.where(bit, src, table[k][v]))
                moved.append(row)
            table = moved
        for b in range(4, 7):
            d = 1 << (b - 4)
            bit = ((shift >> b) & 1) == 1
            table = [
                [
                    jnp.where(bit, rows_up(table[k][v], table[min(k + 1, len(table) - 1)][v], d, s_io), table[k][v])
                    for v in range(NV)
                ]
                for k in range(2)
            ]
        rows = list(table[0])
        for q in range(4):
            tail = table[1][4 * q]
            for u in range(1, 4):
                tail = jnp.where(s_io >= 2 * u, pltpu.roll(table[1][4 * q + u], 2 * u, 0), tail)
            rows.append(tail)
        moved_words.append(rows)
    key, first, second = moved_words
    split = [
        [release(right(x, 11)) for x in first],
        [release(right(x, 11)) for x in second],
        [release(((x & 2047) << 10) | (y & 1023)) for x, y in zip(first, second)],
        [((x >> 14) & 127).astype(jnp.float32) for x in key],
    ]
    for a in range(4):
        send_ref[a] = jnp.concatenate(split[a][:NV], axis=0).T
    send_ref[4] = jnp.concatenate([x for a in range(4) for x in split[a][NV:]], axis=0).T


def return_kernel(back_ref, key_ref, meta_ref, out_ref):
    s_io, l_io = iotas()
    column, shift = meta_ref[0], meta_ref[1]
    keys = [key_ref[v] for v in range(NV)]
    ranks = [x >> 21 for x in keys]
    blocks = [l_io - take_lanes(column, x) for x in ranks]
    tails = back_ref[4].T
    values = []
    for f in range(4):
        main = back_ref[f].T
        first = [main[8 * v : 8 * v + 8] for v in range(NV)]
        second = []
        for v in range(NV):
            q, u = v // 4, v % 4
            at = f * 32 + q * 8
            x = tails[at : at + 8]
            second.append(pltpu.roll(x, 8 - 2 * u, 0) if u else x)
        table = [first, second, second]
        for b in range(6, 3, -1):
            d = 1 << (b - 4)
            bit = ((shift >> b) & 1) == 1
            table = [
                [jnp.where(bit, rows_down(table[max(k - 1, 0)][v], table[k][v], d, s_io), table[k][v]) for v in range(NV)]
                for k in range(3)
            ]
        for b in range(3, -1, -1):
            d = 1 << b
            bit = ((shift >> b) & 1) == 1
            moved = []
            for k in range(3):
                row = []
                for v in range(NV):
                    if v >= d:
                        src = table[k][v - d]
                    else:
                        src = rows_down(table[max(k - 1, 0)][v - d + NV], table[k][v - d + NV], 1, s_io)
                    row.append(jnp.where(bit, src, table[k][v]))
                moved.append(row)
            table = moved
        picked = []
        for v in range(NV):
            x = [take_lanes(table[k][v], ranks[v]) for k in range(3)]
            picked.append(jnp.where(blocks[v] == 0, x[0], jnp.where(blocks[v] == 1, x[1], x[2])))
        values.append(picked)
    largest = functools.reduce(jnp.maximum, [jnp.abs(x) for picked in values for x in picked])
    largest = jnp.maximum(jnp.max(jnp.max(largest, axis=0, keepdims=True), axis=1, keepdims=True), 1e-30)
    grow = jnp.broadcast_to(524287.0 / largest, (8, 128))
    shrink = jnp.broadcast_to(largest / 524287.0, (8, 128))
    words = [[], [], []]
    for v in range(NV):
        q = [(values[f][v] * grow + 524288.5).astype(jnp.int32) for f in range(4)]
        low = ((q[0] & 15) << 12) | ((q[1] & 15) << 8) | ((q[2] & 15) << 4) | (q[3] & 15)
        words[0].append(((keys[v] & 16383) << 16) | low)
        words[1].append(((q[0] >> 4) << 16) | (q[1] >> 4))
        words[2].append(((q[2] >> 4) << 16) | (q[3] >> 4))
    words = network(words)
    for v in range(NV):
        low, first, second = [words[a][v] for a in range(3)]
        q = [
            (right(first, 16) << 4) | ((low >> 12) & 15),
            ((first & 65535) << 4) | ((low >> 8) & 15),
            (right(second, 16) << 4) | ((low >> 4) & 15),
            ((second & 65535) << 4) | (low & 15),
        ]
        for f in range(4):
            out_ref[8 * v : 8 * v + 8, f, :] = (q[f] - 524288).astype(jnp.float32) * shrink


def node_weights(coord):
    node = lax.broadcasted_iota(jnp.int32, (8, coord.shape[1]), 0)
    scale = jnp.full(node.shape, float(gll_scale[0]), jnp.float32)
    for a in range(1, 8):
        scale = jnp.where(node == a, float(gll_scale[a]), scale)
    factors = [jnp.where(node == b, 1.0, coord - float(gll_points[b])) for b in range(8)]
    while len(factors) > 1:
        factors = [factors[i] * factors[i + 1] for i in range(0, len(factors), 2)]
    return factors[0] * scale


def hops(step):
    ring = (0, 1, 2, 1)
    dx, dy, dz = step
    return ring[dx] + ring[dy] + (ring[dz // 2] + ring[(dz + 1) // 2 % 4]) / 2


def slot_order():
    order = sorted(((x, y, z) for x in range(4) for y in range(4) for z in range(8)), key=hops)
    return order[16:64] + order[96:] + order[64:96] + order[:16]


CHUNKS = (16, 32, 32, 32, 16)
STEPS = slot_order()
OWN = STEPS.index((0, 0, 0))


def fill_table(fields, table):
    q = lax.broadcasted_iota(jnp.int32, (256, 256), 0)
    k = lax.broadcasted_iota(jnp.int32, (256, 256), 1)
    mover = ((q % 32) * 8 + q // 32 == k).astype(jnp.float32).astype(jnp.bfloat16)
    for g in range(8):
        block = lax.dot_general(
            mover,
            fields[:, g * 256 : g * 256 + 256],
            (((1,), (1,)), ((), ())),
            preferred_element_type=jnp.float32,
        ).astype(jnp.bfloat16)
        for c in range(8):
            table[g * 32 : g * 32 + 32, c * 128 : c * 128 + 128] = block[c * 32 : c * 32 + 32]


def exchange_kernel(
    rank_hbm,
    slot_hbm,
    coord_hbm,
    fields_hbm,
    back,
    key_ref,
    meta_ref,
    rank_ref,
    slot_ref,
    coord_ref,
    fields,
    send,
    got,
    vals,
    table,
    load_sems,
    send_sem,
    got_sems,
    value_sem,
    back_sem,
):
    gx, gy, gz = (lax.axis_index(name) for name in AXES)
    me = gx * 32 + gy * 8 + gz
    xs = [((gx + k) % 4) * 32 for k in range(4)]
    ys = [((gy + k) % 4) * 8 for k in range(4)]
    zs = [(gz + k) % 8 for k in range(8)]

    def ahead(slot):
        dx, dy, dz = STEPS[slot]
        return xs[dx] + ys[dy] + zs[dz]

    def behind(slot):
        dx, dy, dz = STEPS[slot]
        return xs[-dx % 4] + ys[-dy % 4] + zs[-dz % 8]

    barrier = pltpu.get_barrier_semaphore()
    others = [slot for slot in range(128) if slot != OWN]

    def greet():
        for slot in others:
            pl.semaphore_signal(barrier, inc=1, device_id=ahead(slot), device_id_type=LOGICAL)

    loads = [
        pltpu.make_async_copy(source, place, load_sems.at[i])
        for i, (source, place) in enumerate(
            [(rank_hbm, rank_ref), (slot_hbm, slot_ref), (coord_hbm, coord_ref), (fields_hbm, fields)]
        )
    ]
    for load in loads:
        load.start()
    greet()
    for load in loads:
        load.wait()
    fill_table(fields, table)
    dispatch_steps(rank_ref, slot_ref, coord_ref, send, key_ref, meta_ref)
    pl.semaphore_wait(barrier, 127)

    starts = [sum(CHUNKS[:i]) for i in range(len(CHUNKS))]
    chunk_of = [i for i, count in enumerate(CHUNKS) for _ in range(count)]

    def ship(slot):
        if slot == OWN:
            pltpu.make_async_copy(
                send.at[:, pl.ds(me, 1)], got.at[:, pl.ds(slot, 1)], got_sems.at[chunk_of[slot]]
            ).start()
            return
        where = ahead(slot)
        pltpu.make_async_remote_copy(
            src_ref=send.at[:, pl.ds(where, 1)],
            dst_ref=got.at[:, pl.ds(slot, 1)],
            send_sem=send_sem,
            recv_sem=got_sems.at[chunk_of[slot]],
            device_id=where,
            device_id_type=LOGICAL,
        ).start()

    def answer(slot):
        if slot == OWN:
            pltpu.make_async_copy(vals.at[:, pl.ds(slot, 1)], back.at[:, pl.ds(me, 1)], back_sem).start()
            return
        pltpu.make_async_remote_copy(
            src_ref=vals.at[:, pl.ds(slot, 1)],
            dst_ref=back.at[:, pl.ds(me, 1)],
            send_sem=value_sem,
            recv_sem=back_sem,
            device_id=behind(slot),
            device_id_type=LOGICAL,
        ).start()

    for slot in range(128):
        ship(slot)

    lane = lax.broadcasted_iota(jnp.int32, (1, 128), 1) >> 5
    element = lax.broadcasted_iota(jnp.int32, (128, 256), 0)

    def pair(rows):
        r, s, t, slot = [jnp.concatenate([rows[0][a], rows[1][a]], axis=1) for a in range(4)]
        weight_r, weight_s, weight_t = node_weights(r), node_weights(s), node_weights(t)
        onehot = (element == slot.astype(jnp.int32)).astype(jnp.float32).astype(jnp.bfloat16)
        onehot = onehot.reshape(8, 16, 256)
        parts = []
        for c in range(8):
            w = jnp.broadcast_to(weight_t[c : c + 1], (16, 256)).astype(jnp.bfloat16)
            parts.append((onehot * w[None]).reshape(128, 256))
        along = jnp.dot(table[...], jnp.concatenate(parts, axis=0), preferred_element_type=jnp.float32)
        along = along.reshape(4, 8, 8, 256)
        along = jnp.sum(along * weight_r[None, :, None, :], axis=1)
        value = jnp.sum(along * weight_s[None], axis=1)
        return [[value[f : f + 1, 128 * h : 128 * h + 128] for f in range(4)] for h in range(2)]

    for chunk, count in enumerate(CHUNKS):
        base = starts[chunk]
        block = got.at[:, pl.ds(base, count)]
        pltpu.make_async_copy(block, block, got_sems.at[chunk]).wait()
        tails = []
        for i in range(count // 4):
            ends = [got[4, base + 4 * i + w : base + 4 * i + w + 1, :] for w in range(4)]
            tail = []
            for a in range(4):
                row = None
                for w in range(4):
                    turn = (32 * (w - a)) % 128
                    x = pltpu.roll(ends[w], turn, 1) if turn else ends[w]
                    row = x if row is None else jnp.where(lane == w, x, row)
                tail.append(row)
            tails.append(tail)
        found = []
        for i in range(0, count // 4, 2):
            found += pair(tails[i : i + 2])
        for i in range(count // 4):
            for w in range(4):
                row = None
                for f in range(4):
                    turn = (32 * (f - w)) % 128
                    x = pltpu.roll(found[i][f], turn, 1) if turn else found[i][f]
                    row = x if row is None else jnp.where(lane == f, x, row)
                vals[4, base + 4 * i + w : base + 4 * i + w + 1, :] = row
        for i in range(base, base + count, 2):
            found = pair([[got[a, i + h : i + h + 1, :] for a in range(4)] for h in range(2)])
            for h in range(2):
                for f in range(4):
                    vals[f, i + h : i + h + 1, :] = found[h][f]
        for i in range(base, base + count):
            answer(i)
    sent = send.at[:, pl.ds(0, 127)]
    pltpu.make_async_copy(sent, sent, send_sem).wait()
    told = vals.at[:, pl.ds(0, 127)]
    pltpu.make_async_copy(told, told, value_sem).wait()
    pltpu.make_async_copy(back, back, back_sem).wait()


def exchange(rank, slot, coords, fields):
    return pl.pallas_call(
        exchange_kernel,
        in_specs=[pl.BlockSpec(memory_space=pltpu.HBM)] * 4,
        out_specs=[pl.BlockSpec(memory_space=pltpu.VMEM)] * 3,
        out_shape=[
            jax.ShapeDtypeStruct((5, 128, 128), jnp.float32),
            jax.ShapeDtypeStruct((NV, 8, 128), jnp.int32),
            jax.ShapeDtypeStruct((2, 8, 128), jnp.int32),
        ],
        scratch_shapes=[
            pltpu.VMEM((NV, 8, 128), jnp.int32),
            pltpu.VMEM((NV, 8, 128), jnp.int32),
            pltpu.VMEM((128, 3, 128), jnp.float32),
            pltpu.VMEM((128, 2048), jnp.bfloat16),
            pltpu.VMEM((5, 128, 128), jnp.float32),
            pltpu.VMEM((5, 128, 128), jnp.float32),
            pltpu.VMEM((5, 128, 128), jnp.float32),
            pltpu.VMEM((256, 1024), jnp.bfloat16),
            pltpu.SemaphoreType.DMA((4,)),
            pltpu.SemaphoreType.DMA,
            pltpu.SemaphoreType.DMA((len(CHUNKS),)),
            pltpu.SemaphoreType.DMA,
            pltpu.SemaphoreType.DMA,
        ],
        compiler_params=pltpu.CompilerParams(collective_id=0, has_side_effects=True),
        name="exchange",
    )(rank, slot, coords, fields)


def give_back(back, key, meta):
    return pl.pallas_call(
        return_kernel,
        out_shape=jax.ShapeDtypeStruct((128, 4, 128), jnp.float32),
        name="give_back",
    )(back, key, meta)


def local(fields, coordinates, element_rank, element_slot):
    rank = element_rank.reshape(NV, 8, 128)
    slot = element_slot.reshape(NV, 8, 128)
    coords = coordinates.reshape(3, 128, 128).transpose(1, 0, 2)
    back, key, meta = exchange(rank, slot, coords, fields)
    return give_back(back, key, meta).transpose(1, 0, 2).reshape(4, 16384)


def solution(mesh):
    placed = (P(AXES, None), P(None, AXES), P(AXES, None), P(AXES))
    return jax.shard_map(local, mesh=mesh, in_specs=placed, out_specs=P(None, AXES), check_vma=False)
```

```python
import jax
import jax.numpy as jnp
import numpy as np
from jax import lax
from jax.experimental import pallas as pl
from jax.experimental.pallas import tpu as pltpu
from jax.sharding import PartitionSpec as P

AXES = ("gx", "gy", "gz")
LOGICAL = pl.DeviceIdType.LOGICAL
LEVELS = (1 << 21) - 1
NV = 16

gll_points = np.array(
    [
        -1.0,
        -0.8717401485096066,
        -0.5917001814331423,
        -0.2092992179024789,
        0.2092992179024789,
        0.5917001814331423,
        0.8717401485096066,
        1.0,
    ]
)
gll_scale = np.array(
    [1.0 / np.prod([gll_points[a] - gll_points[b] for b in range(8) if b != a]) for a in range(8)]
)


def iotas():
    return lax.broadcasted_iota(jnp.int32, (8, 128), 0), lax.broadcasted_iota(jnp.int32, (8, 128), 1)


def partner(x, axis, d, bit):
    n = x.shape[axis]
    if 2 * d == n:
        return pltpu.roll(x, d, axis)
    if axis == 1:
        idx = lax.broadcasted_iota(jnp.int32, x.shape, 1) ^ d
        return jnp.take_along_axis(x, idx, axis=1)
    return jnp.where(bit, pltpu.roll(x, d, axis), pltpu.roll(x, n - d, axis))


def network(arrs):
    s_io, l_io = iotas()
    arrs = [list(a) for a in arrs]
    count = len(arrs)

    def bit_of(b):
        if b < 7:
            return ((s_io >> (b - 4)) & 1) == 1
        return ((l_io >> (b - 7)) & 1) == 1

    for k in range(1, 15):
        down = bit_of(k) if 4 <= k < 14 else None
        for j in range(k - 1, 3, -1):
            axis, d = (0, 1 << (j - 4)) if j < 7 else (1, 1 << (j - 7))
            upper = bit_of(j)
            flip = upper if down is None else jnp.logical_xor(upper, down)
            for v in range(NV):
                other = [partner(arrs[a][v], axis, d, upper) for a in range(count)]
                take = jnp.logical_xor(arrs[0][v] > other[0], flip)
                for a in range(count):
                    arrs[a][v] = jnp.where(take, other[a], arrs[a][v])
        for j in range(min(k, 4) - 1, -1, -1):
            d = 1 << j
            for v in range(NV):
                if v & d:
                    continue
                w = v | d
                if k < 4 and (v >> k) & 1:
                    swap = arrs[0][v] < arrs[0][w]
                else:
                    swap = arrs[0][v] > arrs[0][w]
                if down is not None:
                    swap = jnp.logical_xor(swap, down)
                for a in range(count):
                    x, y = arrs[a][v], arrs[a][w]
                    arrs[a][v] = jnp.where(swap, y, x)
                    arrs[a][w] = jnp.where(swap, x, y)
    return arrs


def row_bit(b, s_io):
    return ((s_io >> (b - 4)) & 1) == 1


def plan_route(labels, lane_plan, swap_plan):
    s_io, l_io = iotas()
    items = list(labels)
    note = 0

    def lane_bit(b):
        return ((l_io >> (b - 7)) & 1) == 1

    for k in range(1, 15):
        down = None
        if 4 <= k < 14:
            down = row_bit(k, s_io) if k < 7 else lane_bit(k)
        origin = [l_io] * NV
        for j in range(k - 1, 6, -1):
            upper = lane_bit(j)
            flip = upper if down is None else jnp.logical_xor(upper, down)
            for v in range(NV):
                other = partner(items[v], 1, 1 << (j - 7), upper)
                there = partner(origin[v], 1, 1 << (j - 7), upper)
                take = jnp.logical_xor(items[v] > other, flip)
                items[v] = jnp.where(take, other, items[v])
                origin[v] = jnp.where(take, there, origin[v])
            yield
        if k > 7:
            for v in range(NV):
                lane_plan[k - 8, v] = origin[v]
        for j in range(min(k - 1, 6), 3, -1):
            upper = row_bit(j, s_io)
            flip = upper if down is None else jnp.logical_xor(upper, down)
            for v in range(NV):
                other = partner(items[v], 0, 1 << (j - 4), upper)
                take = jnp.logical_xor(items[v] > other, flip)
                items[v] = jnp.where(take, other, items[v])
                swap_plan[note] = jnp.where(take, 1, 0)
                note += 1
            yield
        for j in range(min(k, 4) - 1, -1, -1):
            d = 1 << j
            for v in range(NV):
                if v & d:
                    continue
                x, y = items[v], items[v | d]
                swap = x < y if k < 4 and (v >> k) & 1 else x > y
                if down is not None:
                    swap = jnp.logical_xor(swap, down)
                items[v], items[v | d] = jnp.where(swap, y, x), jnp.where(swap, x, y)
                swap_plan[note] = jnp.where(swap, 1, 0)
                note += 1
            yield


def follow_route(arrs, lane_plan, swap_plan):
    s_io, _ = iotas()
    arrs = [list(x) for x in arrs]
    note = 0
    for k in range(1, 15):
        if k > 7:
            for v in range(NV):
                idx = lane_plan[k - 8, v]
                for x in arrs:
                    x[v] = take_lanes(x[v], idx)
        for j in range(min(k - 1, 6), 3, -1):
            upper = row_bit(j, s_io)
            for v in range(NV):
                take = swap_plan[note] == 1
                note += 1
                for x in arrs:
                    x[v] = jnp.where(take, partner(x[v], 0, 1 << (j - 4), upper), x[v])
        for j in range(min(k, 4) - 1, -1, -1):
            d = 1 << j
            for v in range(NV):
                if v & d:
                    continue
                swap = swap_plan[note] == 1
                note += 1
                for x in arrs:
                    x[v], x[v | d] = jnp.where(swap, x[v | d], x[v]), jnp.where(swap, x[v], x[v | d])
    return arrs


def take_lanes(x, idx):
    return jnp.take_along_axis(x, idx, axis=1)


def rows_up(low, high, d, s_io):
    return jnp.where(s_io < 8 - d, pltpu.roll(low, 8 - d, 0), pltpu.roll(high, 8 - d, 0))


def rows_down(low, high, d, s_io):
    return jnp.where(s_io >= d, pltpu.roll(high, d, 0), pltpu.roll(low, d, 0))


def hold(x):
    return ((x + 1.0) * (LEVELS / 2) + 0.5).astype(jnp.int32)


def release(q):
    return q.astype(jnp.float32) * (2 / LEVELS) - 1.0


def right(x, count):
    return lax.shift_right_logical(x, jnp.full(x.shape, count, jnp.int32))


def dispatch_steps(rank_ref, slot_ref, coord_ref, send_ref, key_ref, meta_ref):
    s_io, l_io = iotas()
    words = [[], [], []]
    for v in range(NV):
        label = l_io * 128 + s_io * 16 + v
        r, s, t = [hold(coord_ref[8 * v : 8 * v + 8, c, :]) for c in range(3)]
        words[0].append(rank_ref[v] * (1 << 21) + slot_ref[v] * (1 << 14) + label)
        words[1].append((r << 11) | (t >> 10))
        words[2].append((s << 11) | (t & 1023))
    words = network(words)
    keys = words[0]
    for v in range(NV):
        key_ref[v] = keys[v]
    last = (keys[NV - 1][7:8, :] >> 21).astype(jnp.float32)
    last = jnp.broadcast_to(last, (128, 128)).T
    lanes = lax.broadcasted_iota(jnp.int32, (128, 128), 1).astype(jnp.float32)
    column = jnp.sum((last < lanes).astype(jnp.float32), axis=0, keepdims=True)
    column = jnp.broadcast_to(column, (8, 128)).astype(jnp.int32)
    columns = [jnp.minimum(column + k, 127) for k in range(3)]
    spread = [[take_lanes(keys[v], columns[k]) for v in range(NV)] for k in range(3)]
    below = jnp.zeros((8, 128), jnp.float32)
    for v in range(NV):
        below = below + ((spread[0][v] >> 21) < l_io).astype(jnp.float32)
    shift = jnp.broadcast_to(jnp.sum(below, axis=0, keepdims=True), (8, 128)).astype(jnp.int32)
    meta_ref[0] = column
    meta_ref[1] = shift

    moved_words = []
    for a in range(3):
        table = spread if a == 0 else [[take_lanes(words[a][v], columns[k]) for v in range(NV)] for k in range(3)]
        for b in range(4):
            d = 1 << b
            bit = ((shift >> b) & 1) == 1
            moved = []
            for k in range(3):
                row = []
                for v in range(NV):
                    if v + d < NV:
                        src = table[k][v + d]
                    else:
                        src = rows_up(table[k][v + d - NV], table[min(k + 1, 2)][v + d - NV], 1, s_io)
                    row.append(jnp.where(bit, src, table[k][v]))
                moved.append(row)
            table = moved
        for b in range(4, 7):
            d = 1 << (b - 4)
            bit = ((shift >> b) & 1) == 1
            table = [
                [
                    jnp.where(bit, rows_up(table[k][v], table[min(k + 1, len(table) - 1)][v], d, s_io), table[k][v])
                    for v in range(NV)
                ]
                for k in range(2)
            ]
        rows = list(table[0])
        for q in range(4):
            tail = table[1][4 * q]
            for u in range(1, 4):
                tail = jnp.where(s_io >= 2 * u, pltpu.roll(table[1][4 * q + u], 2 * u, 0), tail)
            rows.append(tail)
        moved_words.append(rows)
    key, first, second = moved_words
    split = [
        [release(right(x, 11)) for x in first],
        [release(right(x, 11)) for x in second],
        [release(((x & 2047) << 10) | (y & 1023)) for x, y in zip(first, second)],
        [((x >> 14) & 127).astype(jnp.float32) for x in key],
    ]
    for a in range(4):
        send_ref[a] = jnp.concatenate(split[a][:NV], axis=0).T
    send_ref[4] = jnp.concatenate([x for a in range(4) for x in split[a][NV:]], axis=0).T


def return_steps(back_ref, key_ref, meta_ref, out_ref, lane_plan, swap_plan):
    s_io, l_io = iotas()
    column, shift = meta_ref[0], meta_ref[1]
    keys = [key_ref[v] for v in range(NV)]
    ranks = [x >> 21 for x in keys]
    blocks = [l_io - take_lanes(column, x) for x in ranks]
    tails = back_ref[4].T
    values = []
    for f in range(4):
        main = back_ref[f].T
        first = [main[8 * v : 8 * v + 8] for v in range(NV)]
        second = []
        for v in range(NV):
            q, u = v // 4, v % 4
            at = f * 32 + q * 8
            x = tails[at : at + 8]
            second.append(pltpu.roll(x, 8 - 2 * u, 0) if u else x)
        table = [first, second, second]
        for b in range(6, 3, -1):
            d = 1 << (b - 4)
            bit = ((shift >> b) & 1) == 1
            table = [
                [jnp.where(bit, rows_down(table[max(k - 1, 0)][v], table[k][v], d, s_io), table[k][v]) for v in range(NV)]
                for k in range(3)
            ]
        for b in range(3, -1, -1):
            d = 1 << b
            bit = ((shift >> b) & 1) == 1
            moved = []
            for k in range(3):
                row = []
                for v in range(NV):
                    if v >= d:
                        src = table[k][v - d]
                    else:
                        src = rows_down(table[max(k - 1, 0)][v - d + NV], table[k][v - d + NV], 1, s_io)
                    row.append(jnp.where(bit, src, table[k][v]))
                moved.append(row)
            table = moved
        picked = []
        for v in range(NV):
            x = [take_lanes(table[k][v], ranks[v]) for k in range(3)]
            picked.append(jnp.where(blocks[v] == 0, x[0], jnp.where(blocks[v] == 1, x[1], x[2])))
        values.append(picked)
    values = follow_route(values, lane_plan, swap_plan)
    for f in range(4):
        for v in range(NV):
            out_ref[8 * v : 8 * v + 8, f, :] = values[f][v]


def node_weights(coord):
    node = lax.broadcasted_iota(jnp.int32, (8, coord.shape[1]), 0)
    scale = jnp.full(node.shape, float(gll_scale[0]), jnp.float32)
    for a in range(1, 8):
        scale = jnp.where(node == a, float(gll_scale[a]), scale)
    factors = [jnp.where(node == b, 1.0, coord - float(gll_points[b])) for b in range(8)]
    while len(factors) > 1:
        factors = [factors[i] * factors[i + 1] for i in range(0, len(factors), 2)]
    return factors[0] * scale


def hops(step):
    ring = (0, 1, 2, 1)
    dx, dy, dz = step
    return ring[dx] + ring[dy] + (ring[dz // 2] + ring[(dz + 1) // 2 % 4]) / 2


def slot_order():
    order = sorted(((x, y, z) for x in range(4) for y in range(4) for z in range(8)), key=hops)
    return order[16:64] + order[96:] + order[64:96] + order[:16]


CHUNKS = (16, 32, 32, 32, 16)
PLAN_STEPS = 2
STEPS = slot_order()
OWN = STEPS.index((0, 0, 0))


def fill_table(fields, table):
    q = lax.broadcasted_iota(jnp.int32, (256, 256), 0)
    k = lax.broadcasted_iota(jnp.int32, (256, 256), 1)
    mover = ((q % 32) * 8 + q // 32 == k).astype(jnp.float32).astype(jnp.bfloat16)
    for g in range(8):
        block = lax.dot_general(
            mover,
            fields[:, g * 256 : g * 256 + 256],
            (((1,), (1,)), ((), ())),
            preferred_element_type=jnp.float32,
        ).astype(jnp.bfloat16)
        for c in range(8):
            table[g * 32 : g * 32 + 32, c * 128 : c * 128 + 128] = block[c * 32 : c * 32 + 32]


def exchange_kernel(
    rank_hbm,
    slot_hbm,
    coord_hbm,
    fields_hbm,
    out_ref,
    back,
    key_ref,
    meta_ref,
    rank_ref,
    slot_ref,
    coord_ref,
    fields,
    send,
    got,
    vals,
    table,
    lane_plan,
    swap_plan,
    load_sems,
    send_sem,
    got_sems,
    value_sem,
    back_sem,
):
    gx, gy, gz = (lax.axis_index(name) for name in AXES)
    me = gx * 32 + gy * 8 + gz
    xs = [((gx + k) % 4) * 32 for k in range(4)]
    ys = [((gy + k) % 4) * 8 for k in range(4)]
    zs = [(gz + k) % 8 for k in range(8)]

    def ahead(slot):
        dx, dy, dz = STEPS[slot]
        return xs[dx] + ys[dy] + zs[dz]

    def behind(slot):
        dx, dy, dz = STEPS[slot]
        return xs[-dx % 4] + ys[-dy % 4] + zs[-dz % 8]

    barrier = pltpu.get_barrier_semaphore()
    others = [slot for slot in range(128) if slot != OWN]

    def greet():
        for slot in others:
            pl.semaphore_signal(barrier, inc=1, device_id=ahead(slot), device_id_type=LOGICAL)

    loads = [
        pltpu.make_async_copy(source, place, load_sems.at[i])
        for i, (source, place) in enumerate(
            [(rank_hbm, rank_ref), (slot_hbm, slot_ref), (coord_hbm, coord_ref), (fields_hbm, fields)]
        )
    ]
    for load in loads:
        load.start()
    greet()
    for load in loads:
        load.wait()
    fill_table(fields, table)
    dispatch_steps(rank_ref, slot_ref, coord_ref, send, key_ref, meta_ref)
    pl.semaphore_wait(barrier, 127)

    starts = [sum(CHUNKS[:i]) for i in range(len(CHUNKS))]
    chunk_of = [i for i, count in enumerate(CHUNKS) for _ in range(count)]

    def ship(slot):
        if slot == OWN:
            pltpu.make_async_copy(
                send.at[:, pl.ds(me, 1)], got.at[:, pl.ds(slot, 1)], got_sems.at[chunk_of[slot]]
            ).start()
            return
        where = ahead(slot)
        pltpu.make_async_remote_copy(
            src_ref=send.at[:, pl.ds(where, 1)],
            dst_ref=got.at[:, pl.ds(slot, 1)],
            send_sem=send_sem,
            recv_sem=got_sems.at[chunk_of[slot]],
            device_id=where,
            device_id_type=LOGICAL,
        ).start()

    def answer(slot):
        if slot == OWN:
            pltpu.make_async_copy(vals.at[:, pl.ds(slot, 1)], back.at[:, pl.ds(me, 1)], back_sem).start()
            return
        pltpu.make_async_remote_copy(
            src_ref=vals.at[:, pl.ds(slot, 1)],
            dst_ref=back.at[:, pl.ds(me, 1)],
            send_sem=value_sem,
            recv_sem=back_sem,
            device_id=behind(slot),
            device_id_type=LOGICAL,
        ).start()

    for slot in range(128):
        ship(slot)

    lane = lax.broadcasted_iota(jnp.int32, (1, 128), 1) >> 5
    element = lax.broadcasted_iota(jnp.int32, (128, 256), 0)

    planning = plan_route([key_ref[v] & 16383 for v in range(NV)], lane_plan, swap_plan)

    def pair(rows):
        for _ in range(PLAN_STEPS):
            next(planning, None)
        r, s, t, slot = [jnp.concatenate([rows[0][a], rows[1][a]], axis=1) for a in range(4)]
        weight_r, weight_s, weight_t = node_weights(r), node_weights(s), node_weights(t)
        onehot = (element == slot.astype(jnp.int32)).astype(jnp.float32).astype(jnp.bfloat16)
        onehot = onehot.reshape(8, 16, 256)
        parts = []
        for c in range(8):
            w = jnp.broadcast_to(weight_t[c : c + 1], (16, 256)).astype(jnp.bfloat16)
            parts.append((onehot * w[None]).reshape(128, 256))
        along = jnp.dot(table[...], jnp.concatenate(parts, axis=0), preferred_element_type=jnp.float32)
        along = along.reshape(4, 8, 8, 256)
        along = jnp.sum(along * weight_r[None, :, None, :], axis=1)
        value = jnp.sum(along * weight_s[None], axis=1)
        return [[value[f : f + 1, 128 * h : 128 * h + 128] for f in range(4)] for h in range(2)]

    for chunk, count in enumerate(CHUNKS):
        base = starts[chunk]
        block = got.at[:, pl.ds(base, count)]
        pltpu.make_async_copy(block, block, got_sems.at[chunk]).wait()
        tails = []
        for i in range(count // 4):
            ends = [got[4, base + 4 * i + w : base + 4 * i + w + 1, :] for w in range(4)]
            tail = []
            for a in range(4):
                row = None
                for w in range(4):
                    turn = (32 * (w - a)) % 128
                    x = pltpu.roll(ends[w], turn, 1) if turn else ends[w]
                    row = x if row is None else jnp.where(lane == w, x, row)
                tail.append(row)
            tails.append(tail)
        found = []
        for i in range(0, count // 4, 2):
            found += pair(tails[i : i + 2])
        for i in range(count // 4):
            for w in range(4):
                row = None
                for f in range(4):
                    turn = (32 * (f - w)) % 128
                    x = pltpu.roll(found[i][f], turn, 1) if turn else found[i][f]
                    row = x if row is None else jnp.where(lane == f, x, row)
                vals[4, base + 4 * i + w : base + 4 * i + w + 1, :] = row
        for i in range(base, base + count, 2):
            found = pair([[got[a, i + h : i + h + 1, :] for a in range(4)] for h in range(2)])
            for h in range(2):
                for f in range(4):
                    vals[f, i + h : i + h + 1, :] = found[h][f]
        for i in range(base, base + count):
            answer(i)
    sent = send.at[:, pl.ds(0, 127)]
    pltpu.make_async_copy(sent, sent, send_sem).wait()
    told = vals.at[:, pl.ds(0, 127)]
    pltpu.make_async_copy(told, told, value_sem).wait()
    pltpu.make_async_copy(back, back, back_sem).wait()
    return_steps(back, key_ref, meta_ref, out_ref, lane_plan, swap_plan)


def exchange(rank, slot, coords, fields):
    return pl.pallas_call(
        exchange_kernel,
        in_specs=[pl.BlockSpec(memory_space=pltpu.HBM)] * 4,
        out_specs=pl.BlockSpec(memory_space=pltpu.VMEM),
        out_shape=jax.ShapeDtypeStruct((128, 4, 128), jnp.float32),
        scratch_shapes=[
            pltpu.VMEM((5, 128, 128), jnp.float32),
            pltpu.VMEM((NV, 8, 128), jnp.int32),
            pltpu.VMEM((2, 8, 128), jnp.int32),
            pltpu.VMEM((NV, 8, 128), jnp.int32),
            pltpu.VMEM((NV, 8, 128), jnp.int32),
            pltpu.VMEM((128, 3, 128), jnp.float32),
            pltpu.VMEM((128, 2048), jnp.bfloat16),
            pltpu.VMEM((5, 128, 128), jnp.float32),
            pltpu.VMEM((5, 128, 128), jnp.float32),
            pltpu.VMEM((5, 128, 128), jnp.float32),
            pltpu.VMEM((256, 1024), jnp.bfloat16),
            pltpu.VMEM((7, NV, 8, 128), jnp.int32),
            pltpu.VMEM((832, 8, 128), jnp.int32),
            pltpu.SemaphoreType.DMA((4,)),
            pltpu.SemaphoreType.DMA,
            pltpu.SemaphoreType.DMA((len(CHUNKS),)),
            pltpu.SemaphoreType.DMA,
            pltpu.SemaphoreType.DMA,
        ],
        compiler_params=pltpu.CompilerParams(collective_id=0, has_side_effects=True),
        name="exchange",
    )(rank, slot, coords, fields)


def local(fields, coordinates, element_rank, element_slot):
    rank = element_rank.reshape(NV, 8, 128)
    slot = element_slot.reshape(NV, 8, 128)
    coords = coordinates.reshape(3, 128, 128).transpose(1, 0, 2)
    return exchange(rank, slot, coords, fields).transpose(1, 0, 2).reshape(4, 16384)


def solution(mesh):
    placed = (P(AXES, None), P(None, AXES), P(AXES, None), P(AXES))
    return jax.shard_map(local, mesh=mesh, in_specs=placed, out_specs=P(None, AXES), check_vma=False)
```

```python
import jax
import jax.numpy as jnp
import numpy as np
from jax import lax
from jax.experimental import pallas as pl
from jax.experimental.pallas import tpu as pltpu
from jax.sharding import PartitionSpec as P

AXES = ("gx", "gy", "gz")
LOGICAL = pl.DeviceIdType.LOGICAL
LEVELS = (1 << 21) - 1
NV = 16

gll_points = np.array(
    [
        -1.0,
        -0.8717401485096066,
        -0.5917001814331423,
        -0.2092992179024789,
        0.2092992179024789,
        0.5917001814331423,
        0.8717401485096066,
        1.0,
    ]
)
gll_scale = np.array(
    [1.0 / np.prod([gll_points[a] - gll_points[b] for b in range(8) if b != a]) for a in range(8)]
)


def iotas():
    return lax.broadcasted_iota(jnp.int32, (8, 128), 0), lax.broadcasted_iota(jnp.int32, (8, 128), 1)


def partner(x, axis, d, bit):
    n = x.shape[axis]
    if 2 * d == n:
        return pltpu.roll(x, d, axis)
    if axis == 1:
        idx = lax.broadcasted_iota(jnp.int32, x.shape, 1) ^ d
        return jnp.take_along_axis(x, idx, axis=1)
    return jnp.where(bit, pltpu.roll(x, d, axis), pltpu.roll(x, n - d, axis))


def network(arrs):
    s_io, l_io = iotas()
    arrs = [list(a) for a in arrs]
    count = len(arrs)

    def bit_of(b):
        if b < 7:
            return ((s_io >> (b - 4)) & 1) == 1
        return ((l_io >> (b - 7)) & 1) == 1

    for k in range(1, 15):
        down = bit_of(k) if 4 <= k < 14 else None
        for j in range(k - 1, 3, -1):
            axis, d = (0, 1 << (j - 4)) if j < 7 else (1, 1 << (j - 7))
            upper = bit_of(j)
            flip = upper if down is None else jnp.logical_xor(upper, down)
            for v in range(NV):
                other = [partner(arrs[a][v], axis, d, upper) for a in range(count)]
                take = jnp.logical_xor(arrs[0][v] > other[0], flip)
                for a in range(count):
                    arrs[a][v] = jnp.where(take, other[a], arrs[a][v])
        for j in range(min(k, 4) - 1, -1, -1):
            d = 1 << j
            for v in range(NV):
                if v & d:
                    continue
                w = v | d
                if k < 4 and (v >> k) & 1:
                    swap = arrs[0][v] < arrs[0][w]
                else:
                    swap = arrs[0][v] > arrs[0][w]
                if down is not None:
                    swap = jnp.logical_xor(swap, down)
                for a in range(count):
                    x, y = arrs[a][v], arrs[a][w]
                    arrs[a][v] = jnp.where(swap, y, x)
                    arrs[a][w] = jnp.where(swap, x, y)
    return arrs


def row_bit(b, s_io):
    return ((s_io >> (b - 4)) & 1) == 1


def plan_route(labels, lane_plan, swap_plan):
    s_io, l_io = iotas()
    items = list(labels)
    note = 0

    def lane_bit(b):
        return ((l_io >> (b - 7)) & 1) == 1

    for k in range(1, 15):
        down = None
        if 4 <= k < 14:
            down = row_bit(k, s_io) if k < 7 else lane_bit(k)
        origin = [l_io] * NV
        for j in range(k - 1, 6, -1):
            upper = lane_bit(j)
            flip = upper if down is None else jnp.logical_xor(upper, down)
            for v in range(NV):
                other = partner(items[v], 1, 1 << (j - 7), upper)
                there = partner(origin[v], 1, 1 << (j - 7), upper)
                take = jnp.logical_xor(items[v] > other, flip)
                items[v] = jnp.where(take, other, items[v])
                origin[v] = jnp.where(take, there, origin[v])
            yield
        if k > 7:
            for v in range(NV):
                lane_plan[k - 8, v] = origin[v]
        for j in range(min(k - 1, 6), 3, -1):
            upper = row_bit(j, s_io)
            flip = upper if down is None else jnp.logical_xor(upper, down)
            for v in range(NV):
                other = partner(items[v], 0, 1 << (j - 4), upper)
                take = jnp.logical_xor(items[v] > other, flip)
                items[v] = jnp.where(take, other, items[v])
                swap_plan[note] = jnp.where(take, 1, 0)
                note += 1
            yield
        for j in range(min(k, 4) - 1, -1, -1):
            d = 1 << j
            for v in range(NV):
                if v & d:
                    continue
                x, y = items[v], items[v | d]
                swap = x < y if k < 4 and (v >> k) & 1 else x > y
                if down is not None:
                    swap = jnp.logical_xor(swap, down)
                items[v], items[v | d] = jnp.where(swap, y, x), jnp.where(swap, x, y)
                swap_plan[note] = jnp.where(swap, 1, 0)
                note += 1
            yield


def follow_route(arrs, lane_plan, swap_plan):
    s_io, _ = iotas()
    arrs = [list(x) for x in arrs]
    note = 0
    for k in range(1, 15):
        if k > 7:
            for v in range(NV):
                idx = lane_plan[k - 8, v]
                for x in arrs:
                    x[v] = take_lanes(x[v], idx)
        for j in range(min(k - 1, 6), 3, -1):
            upper = row_bit(j, s_io)
            for v in range(NV):
                take = swap_plan[note] == 1
                note += 1
                for x in arrs:
                    x[v] = jnp.where(take, partner(x[v], 0, 1 << (j - 4), upper), x[v])
        for j in range(min(k, 4) - 1, -1, -1):
            d = 1 << j
            for v in range(NV):
                if v & d:
                    continue
                swap = swap_plan[note] == 1
                note += 1
                for x in arrs:
                    x[v], x[v | d] = jnp.where(swap, x[v | d], x[v]), jnp.where(swap, x[v], x[v | d])
    return arrs


def take_lanes(x, idx):
    return jnp.take_along_axis(x, idx, axis=1)


def rows_up(low, high, d, s_io):
    return jnp.where(s_io < 8 - d, pltpu.roll(low, 8 - d, 0), pltpu.roll(high, 8 - d, 0))


def rows_down(low, high, d, s_io):
    return jnp.where(s_io >= d, pltpu.roll(high, d, 0), pltpu.roll(low, d, 0))


def hold(x):
    return ((x + 1.0) * (LEVELS / 2) + 0.5).astype(jnp.int32)


def release(q):
    return q.astype(jnp.float32) * (2 / LEVELS) - 1.0


def right(x, count):
    return lax.shift_right_logical(x, jnp.full(x.shape, count, jnp.int32))


def dispatch_steps(rank_ref, slot_ref, coord_ref, send_ref, key_ref, meta_ref):
    s_io, l_io = iotas()
    words = [[], [], []]
    for v in range(NV):
        label = l_io * 128 + s_io * 16 + v
        r, s, t = [hold(coord_ref[8 * v : 8 * v + 8, c, :]) for c in range(3)]
        words[0].append(rank_ref[v] * (1 << 21) + slot_ref[v] * (1 << 14) + label)
        words[1].append((r << 11) | (t >> 10))
        words[2].append((s << 11) | (t & 1023))
    words = network(words)
    keys = words[0]
    for v in range(NV):
        key_ref[v] = keys[v]
    last = (keys[NV - 1][7:8, :] >> 21).astype(jnp.float32)
    last = jnp.broadcast_to(last, (128, 128)).T
    lanes = lax.broadcasted_iota(jnp.int32, (128, 128), 1).astype(jnp.float32)
    column = jnp.sum((last < lanes).astype(jnp.float32), axis=0, keepdims=True)
    column = jnp.broadcast_to(column, (8, 128)).astype(jnp.int32)
    columns = [jnp.minimum(column + k, 127) for k in range(3)]
    spread = [[take_lanes(keys[v], columns[k]) for v in range(NV)] for k in range(3)]
    below = jnp.zeros((8, 128), jnp.float32)
    for v in range(NV):
        below = below + ((spread[0][v] >> 21) < l_io).astype(jnp.float32)
    shift = jnp.broadcast_to(jnp.sum(below, axis=0, keepdims=True), (8, 128)).astype(jnp.int32)
    meta_ref[0] = column
    meta_ref[1] = shift

    moved_words = []
    for a in range(3):
        table = spread if a == 0 else [[take_lanes(words[a][v], columns[k]) for v in range(NV)] for k in range(3)]
        for b in range(4):
            d = 1 << b
            bit = ((shift >> b) & 1) == 1
            moved = []
            for k in range(3):
                row = []
                for v in range(NV):
                    if v + d < NV:
                        src = table[k][v + d]
                    else:
                        src = rows_up(table[k][v + d - NV], table[min(k + 1, 2)][v + d - NV], 1, s_io)
                    row.append(jnp.where(bit, src, table[k][v]))
                moved.append(row)
            table = moved
        for b in range(4, 7):
            d = 1 << (b - 4)
            bit = ((shift >> b) & 1) == 1
            table = [
                [
                    jnp.where(bit, rows_up(table[k][v], table[min(k + 1, len(table) - 1)][v], d, s_io), table[k][v])
                    for v in range(NV)
                ]
                for k in range(2)
            ]
        rows = list(table[0])
        for q in range(4):
            tail = table[1][4 * q]
            for u in range(1, 4):
                tail = jnp.where(s_io >= 2 * u, pltpu.roll(table[1][4 * q + u], 2 * u, 0), tail)
            rows.append(tail)
        moved_words.append(rows)
    key, first, second = moved_words
    split = [
        [release(right(x, 11)) for x in first],
        [release(right(x, 11)) for x in second],
        [release(((x & 2047) << 10) | (y & 1023)) for x, y in zip(first, second)],
        [((x >> 14) & 127).astype(jnp.float32) for x in key],
    ]
    for a in range(4):
        send_ref[a] = jnp.concatenate(split[a][:NV], axis=0).T
    send_ref[4] = jnp.concatenate([x for a in range(4) for x in split[a][NV:]], axis=0).T


def return_steps(back_ref, key_ref, meta_ref, out_ref, lane_plan, swap_plan):
    s_io, l_io = iotas()
    column, shift = meta_ref[0], meta_ref[1]
    keys = [key_ref[v] for v in range(NV)]
    ranks = [x >> 21 for x in keys]
    blocks = [l_io - take_lanes(column, x) for x in ranks]
    tails = back_ref[4].T
    values = []
    for f in range(4):
        main = back_ref[f].T
        first = [main[8 * v : 8 * v + 8] for v in range(NV)]
        second = []
        for v in range(NV):
            q, u = v // 4, v % 4
            at = f * 32 + q * 8
            x = tails[at : at + 8]
            second.append(pltpu.roll(x, 8 - 2 * u, 0) if u else x)
        table = [first, second, second]
        for b in range(6, 3, -1):
            d = 1 << (b - 4)
            bit = ((shift >> b) & 1) == 1
            table = [
                [jnp.where(bit, rows_down(table[max(k - 1, 0)][v], table[k][v], d, s_io), table[k][v]) for v in range(NV)]
                for k in range(3)
            ]
        for b in range(3, -1, -1):
            d = 1 << b
            bit = ((shift >> b) & 1) == 1
            moved = []
            for k in range(3):
                row = []
                for v in range(NV):
                    if v >= d:
                        src = table[k][v - d]
                    else:
                        src = rows_down(table[max(k - 1, 0)][v - d + NV], table[k][v - d + NV], 1, s_io)
                    row.append(jnp.where(bit, src, table[k][v]))
                moved.append(row)
            table = moved
        picked = []
        for v in range(NV):
            x = [take_lanes(table[k][v], ranks[v]) for k in range(3)]
            picked.append(jnp.where(blocks[v] == 0, x[0], jnp.where(blocks[v] == 1, x[1], x[2])))
        values.append(picked)
    values = follow_route(values, lane_plan, swap_plan)
    for f in range(4):
        for v in range(NV):
            out_ref[8 * v : 8 * v + 8, f, :] = values[f][v]


def node_weights(coord):
    node = lax.broadcasted_iota(jnp.int32, (8, coord.shape[1]), 0)
    scale = jnp.full(node.shape, float(gll_scale[0]), jnp.float32)
    for a in range(1, 8):
        scale = jnp.where(node == a, float(gll_scale[a]), scale)
    factors = [jnp.where(node == b, 1.0, coord - float(gll_points[b])) for b in range(8)]
    while len(factors) > 1:
        factors = [factors[i] * factors[i + 1] for i in range(0, len(factors), 2)]
    return factors[0] * scale


def hops(step):
    ring = (0, 1, 2, 1)
    dx, dy, dz = step
    return ring[dx] + ring[dy] + (ring[dz // 2] + ring[(dz + 1) // 2 % 4]) / 2


def slot_order():
    order = sorted(((x, y, z) for x in range(4) for y in range(4) for z in range(8)), key=hops)
    return order[16:64] + order[96:] + order[64:96] + order[:16]


CHUNKS = (16, 32, 32, 32, 16)
PLAN_STEPS = 2
STEPS = slot_order()
OWN = STEPS.index((0, 0, 0))


def fill_table(fields, table):
    q = lax.broadcasted_iota(jnp.int32, (256, 256), 0)
    k = lax.broadcasted_iota(jnp.int32, (256, 256), 1)
    mover = ((q % 32) * 8 + q // 32 == k).astype(jnp.float32).astype(jnp.bfloat16)
    for g in range(8):
        block = lax.dot_general(
            mover,
            fields[:, g * 256 : g * 256 + 256],
            (((1,), (1,)), ((), ())),
            preferred_element_type=jnp.float32,
        ).astype(jnp.bfloat16)
        for c in range(8):
            table[g * 32 : g * 32 + 32, c * 128 : c * 128 + 128] = block[c * 32 : c * 32 + 32]


def exchange_kernel(
    rank_hbm,
    slot_hbm,
    coord_hbm,
    fields_hbm,
    out_ref,
    back,
    key_ref,
    meta_ref,
    rank_ref,
    slot_ref,
    coord_ref,
    fields,
    send,
    got,
    vals,
    table,
    lane_plan,
    swap_plan,
    load_sems,
    send_sem,
    got_sems,
    value_sem,
    back_sem,
):
    gx, gy, gz = (lax.axis_index(name) for name in AXES)
    me = gx * 32 + gy * 8 + gz
    xs = [((gx + k) % 4) * 32 for k in range(4)]
    ys = [((gy + k) % 4) * 8 for k in range(4)]
    zs = [(gz + k) % 8 for k in range(8)]

    def ahead(slot):
        dx, dy, dz = STEPS[slot]
        return xs[dx] + ys[dy] + zs[dz]

    def behind(slot):
        dx, dy, dz = STEPS[slot]
        return xs[-dx % 4] + ys[-dy % 4] + zs[-dz % 8]

    barrier = pltpu.get_barrier_semaphore()
    others = [slot for slot in range(128) if slot != OWN]
    others.sort(key=lambda slot: -hops(STEPS[slot]))

    def greet():
        for slot in others:
            pl.semaphore_signal(barrier, inc=1, device_id=ahead(slot), device_id_type=LOGICAL)

    loads = [
        pltpu.make_async_copy(source, place, load_sems.at[i])
        for i, (source, place) in enumerate(
            [(rank_hbm, rank_ref), (slot_hbm, slot_ref), (coord_hbm, coord_ref), (fields_hbm, fields)]
        )
    ]
    for load in loads:
        load.start()
    greet()
    for load in loads:
        load.wait()
    fill_table(fields, table)
    dispatch_steps(rank_ref, slot_ref, coord_ref, send, key_ref, meta_ref)
    pl.semaphore_wait(barrier, 127)

    starts = [sum(CHUNKS[:i]) for i in range(len(CHUNKS))]
    chunk_of = [i for i, count in enumerate(CHUNKS) for _ in range(count)]

    def ship(slot):
        if slot == OWN:
            pltpu.make_async_copy(
                send.at[:, pl.ds(me, 1)], got.at[:, pl.ds(slot, 1)], got_sems.at[chunk_of[slot]]
            ).start()
            return
        where = ahead(slot)
        pltpu.make_async_remote_copy(
            src_ref=send.at[:, pl.ds(where, 1)],
            dst_ref=got.at[:, pl.ds(slot, 1)],
            send_sem=send_sem,
            recv_sem=got_sems.at[chunk_of[slot]],
            device_id=where,
            device_id_type=LOGICAL,
        ).start()

    def answer(slot):
        if slot == OWN:
            pltpu.make_async_copy(vals.at[:, pl.ds(slot, 1)], back.at[:, pl.ds(me, 1)], back_sem).start()
            return
        pltpu.make_async_remote_copy(
            src_ref=vals.at[:, pl.ds(slot, 1)],
            dst_ref=back.at[:, pl.ds(me, 1)],
            send_sem=value_sem,
            recv_sem=back_sem,
            device_id=behind(slot),
            device_id_type=LOGICAL,
        ).start()

    for slot in range(128):
        ship(slot)

    lane = lax.broadcasted_iota(jnp.int32, (1, 128), 1) >> 5
    element = lax.broadcasted_iota(jnp.int32, (128, 256), 0)

    planning = plan_route([key_ref[v] & 16383 for v in range(NV)], lane_plan, swap_plan)

    def pair(rows):
        for _ in range(PLAN_STEPS):
            next(planning, None)
        r, s, t, slot = [jnp.concatenate([rows[0][a], rows[1][a]], axis=1) for a in range(4)]
        weight_r, weight_s, weight_t = node_weights(r), node_weights(s), node_weights(t)
        onehot = (element == slot.astype(jnp.int32)).astype(jnp.float32).astype(jnp.bfloat16)
        onehot = onehot.reshape(8, 16, 256)
        parts = []
        for c in range(8):
            w = jnp.broadcast_to(weight_t[c : c + 1], (16, 256)).astype(jnp.bfloat16)
            parts.append((onehot * w[None]).reshape(128, 256))
        along = jnp.dot(table[...], jnp.concatenate(parts, axis=0), preferred_element_type=jnp.float32)
        along = along.reshape(4, 8, 8, 256)
        along = jnp.sum(along * weight_r[None, :, None, :], axis=1)
        value = jnp.sum(along * weight_s[None], axis=1)
        return [[value[f : f + 1, 128 * h : 128 * h + 128] for f in range(4)] for h in range(2)]

    for chunk, count in enumerate(CHUNKS):
        base = starts[chunk]
        block = got.at[:, pl.ds(base, count)]
        pltpu.make_async_copy(block, block, got_sems.at[chunk]).wait()
        tails = []
        for i in range(count // 4):
            ends = [got[4, base + 4 * i + w : base + 4 * i + w + 1, :] for w in range(4)]
            tail = []
            for a in range(4):
                row = None
                for w in range(4):
                    turn = (32 * (w - a)) % 128
                    x = pltpu.roll(ends[w], turn, 1) if turn else ends[w]
                    row = x if row is None else jnp.where(lane == w, x, row)
                tail.append(row)
            tails.append(tail)
        found = []
        for i in range(0, count // 4, 2):
            found += pair(tails[i : i + 2])
        for i in range(count // 4):
            for w in range(4):
                row = None
                for f in range(4):
                    turn = (32 * (f - w)) % 128
                    x = pltpu.roll(found[i][f], turn, 1) if turn else found[i][f]
                    row = x if row is None else jnp.where(lane == f, x, row)
                vals[4, base + 4 * i + w : base + 4 * i + w + 1, :] = row
        for i in range(base, base + count, 2):
            found = pair([[got[a, i + h : i + h + 1, :] for a in range(4)] for h in range(2)])
            for h in range(2):
                for f in range(4):
                    vals[f, i + h : i + h + 1, :] = found[h][f]
        for i in sorted(range(base, base + count), key=lambda slot: -hops(STEPS[slot])):
            answer(i)
    pltpu.make_async_copy(back, back, back_sem).wait()
    return_steps(back, key_ref, meta_ref, out_ref, lane_plan, swap_plan)
    sent = send.at[:, pl.ds(0, 127)]
    pltpu.make_async_copy(sent, sent, send_sem).wait()
    told = vals.at[:, pl.ds(0, 127)]
    pltpu.make_async_copy(told, told, value_sem).wait()


def exchange(rank, slot, coords, fields):
    return pl.pallas_call(
        exchange_kernel,
        in_specs=[pl.BlockSpec(memory_space=pltpu.HBM)] * 4,
        out_specs=pl.BlockSpec(memory_space=pltpu.VMEM),
        out_shape=jax.ShapeDtypeStruct((128, 4, 128), jnp.float32),
        scratch_shapes=[
            pltpu.VMEM((5, 128, 128), jnp.float32),
            pltpu.VMEM((NV, 8, 128), jnp.int32),
            pltpu.VMEM((2, 8, 128), jnp.int32),
            pltpu.VMEM((NV, 8, 128), jnp.int32),
            pltpu.VMEM((NV, 8, 128), jnp.int32),
            pltpu.VMEM((128, 3, 128), jnp.float32),
            pltpu.VMEM((128, 2048), jnp.bfloat16),
            pltpu.VMEM((5, 128, 128), jnp.float32),
            pltpu.VMEM((5, 128, 128), jnp.float32),
            pltpu.VMEM((5, 128, 128), jnp.float32),
            pltpu.VMEM((256, 1024), jnp.bfloat16),
            pltpu.VMEM((7, NV, 8, 128), jnp.int32),
            pltpu.VMEM((832, 8, 128), jnp.int32),
            pltpu.SemaphoreType.DMA((4,)),
            pltpu.SemaphoreType.DMA,
            pltpu.SemaphoreType.DMA((len(CHUNKS),)),
            pltpu.SemaphoreType.DMA,
            pltpu.SemaphoreType.DMA,
        ],
        compiler_params=pltpu.CompilerParams(collective_id=0, has_side_effects=True),
        name="exchange",
    )(rank, slot, coords, fields)


def local(fields, coordinates, element_rank, element_slot):
    rank = element_rank.reshape(NV, 8, 128)
    slot = element_slot.reshape(NV, 8, 128)
    coords = coordinates.reshape(3, 128, 128).transpose(1, 0, 2)
    return exchange(rank, slot, coords, fields).transpose(1, 0, 2).reshape(4, 16384)


def solution(mesh):
    placed = (P(AXES, None), P(None, AXES), P(AXES, None), P(AXES))
    return jax.shard_map(local, mesh=mesh, in_specs=placed, out_specs=P(None, AXES), check_vma=False)
```

```python
import jax
import jax.numpy as jnp
import numpy as np
from jax import lax
from jax.experimental import pallas as pl
from jax.experimental.pallas import tpu as pltpu
from jax.sharding import PartitionSpec as P

AXES = ("gx", "gy", "gz")
LOGICAL = pl.DeviceIdType.LOGICAL
LEVELS = (1 << 21) - 1
NV = 16

gll_points = np.array(
    [
        -1.0,
        -0.8717401485096066,
        -0.5917001814331423,
        -0.2092992179024789,
        0.2092992179024789,
        0.5917001814331423,
        0.8717401485096066,
        1.0,
    ]
)
gll_scale = np.array(
    [1.0 / np.prod([gll_points[a] - gll_points[b] for b in range(8) if b != a]) for a in range(8)]
)


def iotas():
    return lax.broadcasted_iota(jnp.int32, (8, 128), 0), lax.broadcasted_iota(jnp.int32, (8, 128), 1)


def partner(x, axis, d, bit):
    n = x.shape[axis]
    if 2 * d == n:
        return pltpu.roll(x, d, axis)
    if axis == 1:
        idx = lax.broadcasted_iota(jnp.int32, x.shape, 1) ^ d
        return jnp.take_along_axis(x, idx, axis=1)
    return jnp.where(bit, pltpu.roll(x, d, axis), pltpu.roll(x, n - d, axis))


def network(arrs, beside):
    s_io, l_io = iotas()
    arrs = [list(a) for a in arrs]
    count = len(arrs)

    def bit_of(b):
        if b < 7:
            return ((s_io >> (b - 4)) & 1) == 1
        return ((l_io >> (b - 7)) & 1) == 1

    for k in range(1, 15):
        beside(k)
        down = bit_of(k) if 4 <= k < 14 else None
        for j in range(k - 1, 3, -1):
            axis, d = (0, 1 << (j - 4)) if j < 7 else (1, 1 << (j - 7))
            upper = bit_of(j)
            flip = upper if down is None else jnp.logical_xor(upper, down)
            for v in range(NV):
                other = [partner(arrs[a][v], axis, d, upper) for a in range(count)]
                take = jnp.logical_xor(arrs[0][v] > other[0], flip)
                for a in range(count):
                    arrs[a][v] = jnp.where(take, other[a], arrs[a][v])
        for j in range(min(k, 4) - 1, -1, -1):
            d = 1 << j
            for v in range(NV):
                if v & d:
                    continue
                w = v | d
                if k < 4 and (v >> k) & 1:
                    swap = arrs[0][v] < arrs[0][w]
                else:
                    swap = arrs[0][v] > arrs[0][w]
                if down is not None:
                    swap = jnp.logical_xor(swap, down)
                for a in range(count):
                    x, y = arrs[a][v], arrs[a][w]
                    arrs[a][v] = jnp.where(swap, y, x)
                    arrs[a][w] = jnp.where(swap, x, y)
    return arrs


def row_bit(b, s_io):
    return ((s_io >> (b - 4)) & 1) == 1


def plan_route(labels, lane_plan, swap_plan):
    s_io, l_io = iotas()
    items = list(labels)
    note = 0

    def lane_bit(b):
        return ((l_io >> (b - 7)) & 1) == 1

    for k in range(1, 15):
        down = None
        if 4 <= k < 14:
            down = row_bit(k, s_io) if k < 7 else lane_bit(k)
        origin = [l_io] * NV
        for j in range(k - 1, 6, -1):
            upper = lane_bit(j)
            flip = upper if down is None else jnp.logical_xor(upper, down)
            for v in range(NV):
                other = partner(items[v], 1, 1 << (j - 7), upper)
                there = partner(origin[v], 1, 1 << (j - 7), upper)
                take = jnp.logical_xor(items[v] > other, flip)
                items[v] = jnp.where(take, other, items[v])
                origin[v] = jnp.where(take, there, origin[v])
            yield
        if k > 7:
            for v in range(NV):
                lane_plan[k - 8, v] = origin[v]
        for j in range(min(k - 1, 6), 3, -1):
            upper = row_bit(j, s_io)
            flip = upper if down is None else jnp.logical_xor(upper, down)
            for v in range(NV):
                other = partner(items[v], 0, 1 << (j - 4), upper)
                take = jnp.logical_xor(items[v] > other, flip)
                items[v] = jnp.where(take, other, items[v])
                swap_plan[note] = jnp.where(take, 1, 0)
                note += 1
            yield
        for j in range(min(k, 4) - 1, -1, -1):
            d = 1 << j
            for v in range(NV):
                if v & d:
                    continue
                x, y = items[v], items[v | d]
                swap = x < y if k < 4 and (v >> k) & 1 else x > y
                if down is not None:
                    swap = jnp.logical_xor(swap, down)
                items[v], items[v | d] = jnp.where(swap, y, x), jnp.where(swap, x, y)
                swap_plan[note] = jnp.where(swap, 1, 0)
                note += 1
            yield


def follow_route(arrs, lane_plan, swap_plan):
    s_io, _ = iotas()
    arrs = [list(x) for x in arrs]
    note = 0
    for k in range(1, 15):
        if k > 7:
            for v in range(NV):
                idx = lane_plan[k - 8, v]
                for x in arrs:
                    x[v] = take_lanes(x[v], idx)
        for j in range(min(k - 1, 6), 3, -1):
            upper = row_bit(j, s_io)
            for v in range(NV):
                take = swap_plan[note] == 1
                note += 1
                for x in arrs:
                    x[v] = jnp.where(take, partner(x[v], 0, 1 << (j - 4), upper), x[v])
        for j in range(min(k, 4) - 1, -1, -1):
            d = 1 << j
            for v in range(NV):
                if v & d:
                    continue
                swap = swap_plan[note] == 1
                note += 1
                for x in arrs:
                    x[v], x[v | d] = jnp.where(swap, x[v | d], x[v]), jnp.where(swap, x[v], x[v | d])
    return arrs


def take_lanes(x, idx):
    return jnp.take_along_axis(x, idx, axis=1)


def rows_up(low, high, d, s_io):
    return jnp.where(s_io < 8 - d, pltpu.roll(low, 8 - d, 0), pltpu.roll(high, 8 - d, 0))


def rows_down(low, high, d, s_io):
    return jnp.where(s_io >= d, pltpu.roll(high, d, 0), pltpu.roll(low, d, 0))


def hold(x):
    return ((x + 1.0) * (LEVELS / 2) + 0.5).astype(jnp.int32)


def release(q):
    return q.astype(jnp.float32) * (2 / LEVELS) - 1.0


def right(x, count):
    return lax.shift_right_logical(x, jnp.full(x.shape, count, jnp.int32))


def dispatch_steps(rank_ref, slot_ref, coord_ref, send_ref, key_ref, meta_ref, beside):
    s_io, l_io = iotas()
    words = [[], [], []]
    for v in range(NV):
        label = l_io * 128 + s_io * 16 + v
        r, s, t = [hold(coord_ref[8 * v : 8 * v + 8, c, :]) for c in range(3)]
        words[0].append(rank_ref[v] * (1 << 21) + slot_ref[v] * (1 << 14) + label)
        words[1].append((r << 11) | (t >> 10))
        words[2].append((s << 11) | (t & 1023))
    words = network(words, beside)
    keys = words[0]
    for v in range(NV):
        key_ref[v] = keys[v]
    last = (keys[NV - 1][7:8, :] >> 21).astype(jnp.float32)
    last = jnp.broadcast_to(last, (128, 128)).T
    lanes = lax.broadcasted_iota(jnp.int32, (128, 128), 1).astype(jnp.float32)
    column = jnp.sum((last < lanes).astype(jnp.float32), axis=0, keepdims=True)
    column = jnp.broadcast_to(column, (8, 128)).astype(jnp.int32)
    columns = [jnp.minimum(column + k, 127) for k in range(3)]
    spread = [[take_lanes(keys[v], columns[k]) for v in range(NV)] for k in range(3)]
    below = jnp.zeros((8, 128), jnp.float32)
    for v in range(NV):
        below = below + ((spread[0][v] >> 21) < l_io).astype(jnp.float32)
    shift = jnp.broadcast_to(jnp.sum(below, axis=0, keepdims=True), (8, 128)).astype(jnp.int32)
    meta_ref[0] = column
    meta_ref[1] = shift

    moved_words = []
    for a in range(3):
        table = spread if a == 0 else [[take_lanes(words[a][v], columns[k]) for v in range(NV)] for k in range(3)]
        for b in range(4):
            d = 1 << b
            bit = ((shift >> b) & 1) == 1
            moved = []
            for k in range(3):
                row = []
                for v in range(NV):
                    if v + d < NV:
                        src = table[k][v + d]
                    else:
                        src = rows_up(table[k][v + d - NV], table[min(k + 1, 2)][v + d - NV], 1, s_io)
                    row.append(jnp.where(bit, src, table[k][v]))
                moved.append(row)
            table = moved
        for b in range(4, 7):
            d = 1 << (b - 4)
            bit = ((shift >> b) & 1) == 1
            table = [
                [
                    jnp.where(bit, rows_up(table[k][v], table[min(k + 1, len(table) - 1)][v], d, s_io), table[k][v])
                    for v in range(NV)
                ]
                for k in range(2)
            ]
        rows = list(table[0])
        for q in range(4):
            tail = table[1][4 * q]
            for u in range(1, 4):
                tail = jnp.where(s_io >= 2 * u, pltpu.roll(table[1][4 * q + u], 2 * u, 0), tail)
            rows.append(tail)
        moved_words.append(rows)
    key, first, second = moved_words
    split = [
        [release(right(x, 11)) for x in first],
        [release(right(x, 11)) for x in second],
        [release(((x & 2047) << 10) | (y & 1023)) for x, y in zip(first, second)],
        [((x >> 14) & 127).astype(jnp.float32) for x in key],
    ]
    for a in range(4):
        send_ref[a] = jnp.concatenate(split[a][:NV], axis=0).T
    send_ref[4] = jnp.concatenate([x for a in range(4) for x in split[a][NV:]], axis=0).T


def return_steps(back_ref, key_ref, meta_ref, out_ref, lane_plan, swap_plan):
    s_io, l_io = iotas()
    column, shift = meta_ref[0], meta_ref[1]
    keys = [key_ref[v] for v in range(NV)]
    ranks = [x >> 21 for x in keys]
    blocks = [l_io - take_lanes(column, x) for x in ranks]
    tails = back_ref[4].T
    values = []
    for f in range(4):
        main = back_ref[f].T
        first = [main[8 * v : 8 * v + 8] for v in range(NV)]
        second = []
        for v in range(NV):
            q, u = v // 4, v % 4
            at = f * 32 + q * 8
            x = tails[at : at + 8]
            second.append(pltpu.roll(x, 8 - 2 * u, 0) if u else x)
        table = [first, second, second]
        for b in range(6, 3, -1):
            d = 1 << (b - 4)
            bit = ((shift >> b) & 1) == 1
            table = [
                [jnp.where(bit, rows_down(table[max(k - 1, 0)][v], table[k][v], d, s_io), table[k][v]) for v in range(NV)]
                for k in range(3)
            ]
        for b in range(3, -1, -1):
            d = 1 << b
            bit = ((shift >> b) & 1) == 1
            moved = []
            for k in range(3):
                row = []
                for v in range(NV):
                    if v >= d:
                        src = table[k][v - d]
                    else:
                        src = rows_down(table[max(k - 1, 0)][v - d + NV], table[k][v - d + NV], 1, s_io)
                    row.append(jnp.where(bit, src, table[k][v]))
                moved.append(row)
            table = moved
        picked = []
        for v in range(NV):
            x = [take_lanes(table[k][v], ranks[v]) for k in range(3)]
            picked.append(jnp.where(blocks[v] == 0, x[0], jnp.where(blocks[v] == 1, x[1], x[2])))
        values.append(picked)
    values = follow_route(values, lane_plan, swap_plan)
    for f in range(4):
        for v in range(NV):
            out_ref[8 * v : 8 * v + 8, f, :] = values[f][v]


def node_weights(coord):
    node = lax.broadcasted_iota(jnp.int32, (8, coord.shape[1]), 0)
    scale = jnp.full(node.shape, float(gll_scale[0]), jnp.float32)
    for a in range(1, 8):
        scale = jnp.where(node == a, float(gll_scale[a]), scale)
    factors = [jnp.where(node == b, 1.0, coord - float(gll_points[b])) for b in range(8)]
    while len(factors) > 1:
        factors = [factors[i] * factors[i + 1] for i in range(0, len(factors), 2)]
    return factors[0] * scale


def hops(step):
    ring = (0, 1, 2, 1)
    dx, dy, dz = step
    return ring[dx] + ring[dy] + (ring[dz // 2] + ring[(dz + 1) // 2 % 4]) / 2


def slot_order():
    order = sorted(((x, y, z) for x in range(4) for y in range(4) for z in range(8)), key=hops)
    return order[16:64] + order[96:] + order[64:96] + order[:16]


CHUNKS = (16, 32, 32, 32, 16)
PLAN_STEPS = 2
STEPS = slot_order()
OWN = STEPS.index((0, 0, 0))


def fill_table(fields, table, g):
    q = lax.broadcasted_iota(jnp.int32, (256, 256), 0)
    k = lax.broadcasted_iota(jnp.int32, (256, 256), 1)
    mover = ((q % 32) * 8 + q // 32 == k).astype(jnp.float32).astype(jnp.bfloat16)
    block = lax.dot_general(
        mover,
        fields[:, g * 256 : g * 256 + 256],
        (((1,), (1,)), ((), ())),
        preferred_element_type=jnp.float32,
    ).astype(jnp.bfloat16)
    for c in range(8):
        table[g * 32 : g * 32 + 32, c * 128 : c * 128 + 128] = block[c * 32 : c * 32 + 32]


def exchange_kernel(
    rank_hbm,
    slot_hbm,
    coord_hbm,
    fields_hbm,
    out_ref,
    back,
    key_ref,
    meta_ref,
    rank_ref,
    slot_ref,
    coord_ref,
    fields,
    send,
    got,
    vals,
    table,
    lane_plan,
    swap_plan,
    load_sems,
    send_sem,
    got_sems,
    value_sem,
    back_sem,
):
    gx, gy, gz = (lax.axis_index(name) for name in AXES)
    me = gx * 32 + gy * 8 + gz
    xs = [((gx + k) % 4) * 32 for k in range(4)]
    ys = [((gy + k) % 4) * 8 for k in range(4)]
    zs = [(gz + k) % 8 for k in range(8)]

    def ahead(slot):
        dx, dy, dz = STEPS[slot]
        return xs[dx] + ys[dy] + zs[dz]

    def behind(slot):
        dx, dy, dz = STEPS[slot]
        return xs[-dx % 4] + ys[-dy % 4] + zs[-dz % 8]

    barrier = pltpu.get_barrier_semaphore()
    others = [slot for slot in range(128) if slot != OWN]
    others.sort(key=lambda slot: -hops(STEPS[slot]))

    def greet():
        for slot in others:
            pl.semaphore_signal(barrier, inc=1, device_id=ahead(slot), device_id_type=LOGICAL)

    loads = [
        pltpu.make_async_copy(source, place, load_sems.at[i])
        for i, (source, place) in enumerate(
            [(rank_hbm, rank_ref), (slot_hbm, slot_ref), (coord_hbm, coord_ref), (fields_hbm, fields)]
        )
    ]
    for load in loads:
        load.start()
    greet()
    for load in loads[:3]:
        load.wait()

    def beside(level):
        if level == 9:
            loads[3].wait()
        if level > 8:
            fill_table(fields, table, level - 9)
        if level == 14:
            fill_table(fields, table, 6)
            fill_table(fields, table, 7)

    dispatch_steps(rank_ref, slot_ref, coord_ref, send, key_ref, meta_ref, beside)
    pl.semaphore_wait(barrier, 127)

    starts = [sum(CHUNKS[:i]) for i in range(len(CHUNKS))]
    chunk_of = [i for i, count in enumerate(CHUNKS) for _ in range(count)]

    def ship(slot):
        if slot == OWN:
            pltpu.make_async_copy(
                send.at[:, pl.ds(me, 1)], got.at[:, pl.ds(slot, 1)], got_sems.at[chunk_of[slot]]
            ).start()
            return
        where = ahead(slot)
        pltpu.make_async_remote_copy(
            src_ref=send.at[:, pl.ds(where, 1)],
            dst_ref=got.at[:, pl.ds(slot, 1)],
            send_sem=send_sem,
            recv_sem=got_sems.at[chunk_of[slot]],
            device_id=where,
            device_id_type=LOGICAL,
        ).start()

    def answer(slot):
        if slot == OWN:
            pltpu.make_async_copy(vals.at[:, pl.ds(slot, 1)], back.at[:, pl.ds(me, 1)], back_sem).start()
            return
        pltpu.make_async_remote_copy(
            src_ref=vals.at[:, pl.ds(slot, 1)],
            dst_ref=back.at[:, pl.ds(me, 1)],
            send_sem=value_sem,
            recv_sem=back_sem,
            device_id=behind(slot),
            device_id_type=LOGICAL,
        ).start()

    for slot in range(128):
        ship(slot)

    lane = lax.broadcasted_iota(jnp.int32, (1, 128), 1) >> 5
    element = lax.broadcasted_iota(jnp.int32, (128, 256), 0)

    planning = plan_route([key_ref[v] & 16383 for v in range(NV)], lane_plan, swap_plan)

    def pair(rows):
        for _ in range(PLAN_STEPS):
            next(planning, None)
        r, s, t, slot = [jnp.concatenate([rows[0][a], rows[1][a]], axis=1) for a in range(4)]
        weight_r, weight_s, weight_t = node_weights(r), node_weights(s), node_weights(t)
        onehot = (element == slot.astype(jnp.int32)).astype(jnp.float32).astype(jnp.bfloat16)
        onehot = onehot.reshape(8, 16, 256)
        parts = []
        for c in range(8):
            w = jnp.broadcast_to(weight_t[c : c + 1], (16, 256)).astype(jnp.bfloat16)
            parts.append((onehot * w[None]).reshape(128, 256))
        along = jnp.dot(table[...], jnp.concatenate(parts, axis=0), preferred_element_type=jnp.float32)
        along = along.reshape(4, 8, 8, 256)
        along = jnp.sum(along * weight_r[None, :, None, :], axis=1)
        value = jnp.sum(along * weight_s[None], axis=1)
        return [[value[f : f + 1, 128 * h : 128 * h + 128] for f in range(4)] for h in range(2)]

    for chunk, count in enumerate(CHUNKS):
        base = starts[chunk]
        block = got.at[:, pl.ds(base, count)]
        pltpu.make_async_copy(block, block, got_sems.at[chunk]).wait()
        tails = []
        for i in range(count // 4):
            ends = [got[4, base + 4 * i + w : base + 4 * i + w + 1, :] for w in range(4)]
            tail = []
            for a in range(4):
                row = None
                for w in range(4):
                    turn = (32 * (w - a)) % 128
                    x = pltpu.roll(ends[w], turn, 1) if turn else ends[w]
                    row = x if row is None else jnp.where(lane == w, x, row)
                tail.append(row)
            tails.append(tail)
        found = []
        for i in range(0, count // 4, 2):
            found += pair(tails[i : i + 2])
        for i in range(count // 4):
            for w in range(4):
                row = None
                for f in range(4):
                    turn = (32 * (f - w)) % 128
                    x = pltpu.roll(found[i][f], turn, 1) if turn else found[i][f]
                    row = x if row is None else jnp.where(lane == f, x, row)
                vals[4, base + 4 * i + w : base + 4 * i + w + 1, :] = row
        for i in range(base, base + count, 2):
            found = pair([[got[a, i + h : i + h + 1, :] for a in range(4)] for h in range(2)])
            for h in range(2):
                for f in range(4):
                    vals[f, i + h : i + h + 1, :] = found[h][f]
        for i in sorted(range(base, base + count), key=lambda slot: -hops(STEPS[slot])):
            answer(i)
    pltpu.make_async_copy(back, back, back_sem).wait()
    return_steps(back, key_ref, meta_ref, out_ref, lane_plan, swap_plan)
    sent = send.at[:, pl.ds(0, 127)]
    pltpu.make_async_copy(sent, sent, send_sem).wait()
    told = vals.at[:, pl.ds(0, 127)]
    pltpu.make_async_copy(told, told, value_sem).wait()


def exchange(rank, slot, coords, fields):
    return pl.pallas_call(
        exchange_kernel,
        in_specs=[pl.BlockSpec(memory_space=pltpu.HBM)] * 4,
        out_specs=pl.BlockSpec(memory_space=pltpu.VMEM),
        out_shape=jax.ShapeDtypeStruct((128, 4, 128), jnp.float32),
        scratch_shapes=[
            pltpu.VMEM((5, 128, 128), jnp.float32),
            pltpu.VMEM((NV, 8, 128), jnp.int32),
            pltpu.VMEM((2, 8, 128), jnp.int32),
            pltpu.VMEM((NV, 8, 128), jnp.int32),
            pltpu.VMEM((NV, 8, 128), jnp.int32),
            pltpu.VMEM((128, 3, 128), jnp.float32),
            pltpu.VMEM((128, 2048), jnp.bfloat16),
            pltpu.VMEM((5, 128, 128), jnp.float32),
            pltpu.VMEM((5, 128, 128), jnp.float32),
            pltpu.VMEM((5, 128, 128), jnp.float32),
            pltpu.VMEM((256, 1024), jnp.bfloat16),
            pltpu.VMEM((7, NV, 8, 128), jnp.int32),
            pltpu.VMEM((832, 8, 128), jnp.int32),
            pltpu.SemaphoreType.DMA((4,)),
            pltpu.SemaphoreType.DMA,
            pltpu.SemaphoreType.DMA((len(CHUNKS),)),
            pltpu.SemaphoreType.DMA,
            pltpu.SemaphoreType.DMA,
        ],
        compiler_params=pltpu.CompilerParams(collective_id=0, has_side_effects=True),
        name="exchange",
    )(rank, slot, coords, fields)


def local(fields, coordinates, element_rank, element_slot):
    rank = element_rank.reshape(NV, 8, 128)
    slot = element_slot.reshape(NV, 8, 128)
    coords = coordinates.reshape(3, 128, 128).transpose(1, 0, 2)
    return exchange(rank, slot, coords, fields).transpose(1, 0, 2).reshape(4, 16384)


def solution(mesh):
    placed = (P(AXES, None), P(None, AXES), P(AXES, None), P(AXES))
    return jax.shard_map(local, mesh=mesh, in_specs=placed, out_specs=P(None, AXES), check_vma=False)
```
